32 devices in a mesh: data: 32 (over z, y, x, core).
Axes of the slice: x: 2, y: 2, z: 4, core: 2. Of those that a mesh axis runs over, the one named last changes fastest.
Arguments:
- tokens: bfloat16 [8192, 1280], P('data')
- labels: int32 [3, 8192], P(None, 'data')
- w_one: bfloat16 [1280, 5120], replicated
- w_two: bfloat16 [5120, 1280], replicated
- adapter_a: bfloat16 [1280, 8], replicated
- adapter_b: bfloat16 [8, 5120], replicated
- task_heads: bfloat16 [3, 1280, 13], replicated
Outputs:
- output 1: float32 [3], replicated
- output 2: float32 [1280, 8], P('data')
- output 3: float32 [8, 5120], P(None, 'data')
All inputs are finite; a program needn't handle non-finite values.
Results may differ from the reference program's by a relative error of at most 0.00237.
Values are sent between devices in bfloat16 or wider.
A program may use at most 1 GiB of HBM per device.

```python
import jax
import jax.numpy as jnp
from jax import lax

DEVICES = 32
TOK_DEV = 256
D_MODEL = 1280
D_FF = 5120
LORA_RANK = 8
NUM_TASKS = 3
NUM_CLASSES = 13
EG_STEPS = 20


def draw_labels(label_key):
    key_list = jax.random.split(label_key, 4)
    total_tok = DEVICES * TOK_DEV
    dev_shift = jax.random.randint(key_list[0], (DEVICES, 1), 0, NUM_CLASSES)
    half_width = (NUM_CLASSES + 1) // 2
    common_lab = (dev_shift + jax.random.randint(key_list[1], (DEVICES, TOK_DEV), 0, half_width)) % NUM_CLASSES
    common_lab = common_lab.reshape(total_tok)
    own_lab = jax.random.randint(key_list[2], (NUM_TASKS, total_tok), 0, NUM_CLASSES)
    pick_common = jax.random.randint(key_list[3], (NUM_TASKS, total_tok), 0, 5) < 3
    return jnp.where(pick_common, common_lab[None, :], own_lab).astype(jnp.int32)


def setup_inputs(seed: int = 0) -> dict:
    key_list = jax.random.split(jax.random.key(seed), 8)
    total_tok = DEVICES * TOK_DEV
    tokens = jax.random.normal(key_list[0], (total_tok, D_MODEL), jnp.float32)
    w_one = jax.random.normal(key_list[1], (D_MODEL, D_FF), jnp.float32) * D_MODEL ** -0.5
    w_two = jax.random.normal(key_list[2], (D_FF, D_MODEL), jnp.float32) * D_FF ** -0.5
    adapter_a = jax.random.normal(key_list[3], (D_MODEL, LORA_RANK), jnp.float32) * D_MODEL ** -0.5
    adapter_b = jax.random.normal(key_list[4], (LORA_RANK, D_FF), jnp.float32) * LORA_RANK ** -0.5
    head_common = jax.random.normal(key_list[5], (D_MODEL, NUM_CLASSES), jnp.float32)
    head_own = jax.random.normal(key_list[6], (NUM_TASKS, D_MODEL, NUM_CLASSES), jnp.float32)
    head_sign = jnp.where(jnp.arange(NUM_TASKS) % 2 == 0, 1.0, -1.0)
    task_heads = (head_sign[:, None, None] * head_common[None] + 0.8 * head_own) * (1.5 * D_MODEL ** -0.5)
    labels = draw_labels(key_list[7])
    return {
        "tokens": tokens.astype(jnp.bfloat16),
        "labels": labels,
        "w_one": w_one.astype(jnp.bfloat16),
        "w_two": w_two.astype(jnp.bfloat16),
        "adapter_a": adapter_a.astype(jnp.bfloat16),
        "adapter_b": adapter_b.astype(jnp.bfloat16),
        "task_heads": task_heads.astype(jnp.bfloat16),
    }


def block_grads(tok_blk, lab_blk, w_one, w_two, adapter_a, adapter_b, task_heads):
    low_rank = jnp.dot(tok_blk, adapter_a, preferred_element_type=jnp.float32).astype(jnp.bfloat16)
    pre_act = jnp.dot(tok_blk, w_one, preferred_element_type=jnp.float32) + jnp.dot(low_rank, adapter_b, preferred_element_type=jnp.float32)
    gelu_out, gelu_slope = jax.jvp(jax.nn.gelu, (pre_act,), (jnp.ones_like(pre_act),))
    hidden = gelu_out.astype(jnp.bfloat16)
    trunk_out = (tok_blk.astype(jnp.float32) + jnp.dot(hidden, w_two, preferred_element_type=jnp.float32)).astype(jnp.bfloat16)
    logits = jnp.einsum("bd,tdc->tbc", trunk_out.astype(jnp.float32), task_heads.astype(jnp.float32))
    task_probs = jax.nn.softmax(logits, axis=-1)
    onehot = (lab_blk[:, :, None] == jnp.arange(NUM_CLASSES)[None, None, :]).astype(jnp.float32)
    logit_err = (task_probs - onehot).astype(jnp.bfloat16)
    d_trunk = jnp.einsum("tbc,tdc->tbd", logit_err.astype(jnp.float32), task_heads.astype(jnp.float32)).astype(jnp.bfloat16)
    d_hidden = jnp.einsum("tbd,fd->tbf", d_trunk.astype(jnp.float32), w_two.astype(jnp.float32))
    d_pre = (d_hidden * gelu_slope[None]).astype(jnp.bfloat16)
    part_b = jnp.einsum("br,tbf->trf", low_rank.astype(jnp.float32), d_pre.astype(jnp.float32))
    d_low = jnp.einsum("tbf,rf->tbr", d_pre.astype(jnp.float32), adapter_b.astype(jnp.float32)).astype(jnp.bfloat16)
    part_a = jnp.einsum("bd,tbr->tdr", tok_blk.astype(jnp.float32), d_low.astype(jnp.float32))
    return part_a, part_b


def reference(tokens, labels, w_one, w_two, adapter_a, adapter_b, task_heads):
    tok_blocks = tokens.reshape(DEVICES, TOK_DEV, D_MODEL)
    lab_blocks = labels.reshape(NUM_TASKS, DEVICES, TOK_DEV).transpose(1, 0, 2)

    def add_block(run_sum, block_in):
        part_a, part_b = block_grads(block_in[0], block_in[1], w_one, w_two, adapter_a, adapter_b, task_heads)
        return (run_sum[0] + part_a, run_sum[1] + part_b), None

    zero_init = (jnp.zeros((NUM_TASKS, D_MODEL, LORA_RANK), jnp.float32), jnp.zeros((NUM_TASKS, LORA_RANK, D_FF), jnp.float32))
    sums, _ = lax.scan(add_block, zero_init, (tok_blocks, lab_blocks))
    batch_total = DEVICES * TOK_DEV
    grad_a = sums[0] / batch_total
    grad_b = sums[1] / batch_total
    gram_mat = jnp.einsum("tdr,sdr->ts", grad_a, grad_a) + jnp.einsum("trf,srf->ts", grad_b, grad_b)
    eg_scale = jnp.trace(gram_mat) / NUM_TASKS

    def eg_step(weights, _):
        weights = weights * jnp.exp(-jnp.sum(gram_mat * weights[None, :], axis=1) / eg_scale)
        return weights / jnp.sum(weights), None

    task_weights, _ = lax.scan(eg_step, jnp.full((NUM_TASKS,), 1.0 / NUM_TASKS, jnp.float32), None, length=EG_STEPS)
    comb_a = jnp.sum(task_weights[:, None, None] * grad_a, axis=0)
    comb_b = jnp.sum(task_weights[:, None, None] * grad_b, axis=0)
    return (task_weights, comb_a, comb_b)
```

```python
import functools

import jax
import jax.numpy as jnp
from jax import lax
from jax.experimental import pallas as pl
from jax.experimental.pallas import tpu as pltpu
from jax.sharding import PartitionSpec as P

EG_STEPS = 20
MESH = pl.DeviceIdType.MESH


def task_grads(tokens, labels, w_one, w_two, adapter_a, adapter_b, task_heads):
    num_classes = task_heads.shape[2]
    low_rank = jnp.dot(tokens, adapter_a, preferred_element_type=jnp.float32).astype(jnp.bfloat16)
    pre_act = jnp.dot(tokens, w_one, preferred_element_type=jnp.float32) + jnp.dot(low_rank, adapter_b, preferred_element_type=jnp.float32)
    gelu_out, gelu_slope = jax.jvp(jax.nn.gelu, (pre_act,), (jnp.ones_like(pre_act),))
    hidden = gelu_out.astype(jnp.bfloat16)
    trunk_out = (tokens.astype(jnp.float32) + jnp.dot(hidden, w_two, preferred_element_type=jnp.float32)).astype(jnp.bfloat16)
    logits = jnp.einsum("bd,tdc->tbc", trunk_out, task_heads, preferred_element_type=jnp.float32)
    task_probs = jax.nn.softmax(logits, axis=-1)
    onehot = (labels[:, :, None] == jnp.arange(num_classes)[None, None, :]).astype(jnp.float32)
    logit_err = (task_probs - onehot).astype(jnp.bfloat16)
    d_trunk = jnp.einsum("tbc,tdc->tbd", logit_err, task_heads, preferred_element_type=jnp.float32).astype(jnp.bfloat16)
    d_hidden = jnp.einsum("tbd,fd->tbf", d_trunk, w_two, preferred_element_type=jnp.float32)
    d_pre = (d_hidden * gelu_slope[None]).astype(jnp.bfloat16)
    part_b = jnp.einsum("cs,ucg->usg", low_rank, d_pre, preferred_element_type=jnp.float32)
    d_low = jnp.einsum("tbf,rf->tbr", d_pre, adapter_b, preferred_element_type=jnp.float32).astype(jnp.bfloat16)
    part_a = jnp.einsum("bd,tbr->tdr", tokens, d_low, preferred_element_type=jnp.float32)
    return part_a, part_b


def pack_parts(part_a, part_b, num_dev):
    main_b = part_b.reshape(3, 8, num_dev, 160)
    rem_b = main_b[..., 128:].transpose(2, 1, 0, 3).reshape(num_dev, 1, 8, 96)
    main_b = main_b[..., :128].transpose(2, 0, 1, 3)
    rows_a = part_a.reshape(3, num_dev, 5, 8, 8).transpose(1, 3, 2, 0, 4).reshape(num_dev, 1, 8, 120)
    rem_b = jnp.pad(rem_b, ((0, 0), (0, 0), (0, 0), (0, 32)))
    rows_a = jnp.pad(rows_a, ((0, 0), (0, 0), (0, 0), (0, 8)))
    return jnp.concatenate([main_b, rem_b, rows_a], axis=1)


def full_sum(tile):
    return jnp.sum(jnp.sum(tile, axis=0, keepdims=True), axis=1, keepdims=True)


def local_gram(main, rem, rows):
    lane = lax.broadcasted_iota(jnp.int32, (8, 128), 1)
    rem_task = lane // 32
    row_task = (lane % 24) // 8
    rem_1, rem_2 = pltpu.roll(rem, 96, 1), pltpu.roll(rem, 64, 1)
    row_1, row_2 = pltpu.roll(rows, 120, 1), pltpu.roll(rows, 112, 1)

    def entry(t, s, rem_other, row_other):
        tile = main[t] * main[s]
        tile = tile + jnp.where(rem_task == t, rem * rem_other, 0.0)
        return full_sum(tile + jnp.where(row_task == t, rows * row_other, 0.0))

    entries = [entry(0, 0, rem, rows), entry(1, 1, rem, rows), entry(2, 2, rem, rows)]
    entries += [entry(0, 1, rem_1, row_1), entry(1, 2, rem_1, row_1), entry(0, 2, rem_2, row_2)]
    lane_row = lax.broadcasted_iota(jnp.int32, (1, 128), 1)
    gram_row = jnp.zeros((1, 128), jnp.float32)
    for k, value in enumerate(entries):
        gram_row = jnp.where(lane_row == k, value, gram_row)
    return gram_row


def solve_weights(gram_row):
    lane_row = lax.broadcasted_iota(jnp.int32, (1, 128), 1)
    m00, m11, m22, m01, m12, m02 = [jnp.sum(jnp.where(lane_row == k, gram_row, 0.0), axis=1, keepdims=True) for k in range(6)]
    scale = (m00 + m11 + m22) / 3.0

    def eg_step(_, w):
        w0, w1, w2 = w
        w0, w1, w2 = (
            w0 * jnp.exp(-(m00 * w0 + m01 * w1 + m02 * w2) / scale),
            w1 * jnp.exp(-(m01 * w0 + m11 * w1 + m12 * w2) / scale),
            w2 * jnp.exp(-(m02 * w0 + m12 * w1 + m22 * w2) / scale),
        )
        total = w0 + w1 + w2
        return w0 / total, w1 / total, w2 / total

    third = jnp.full((1, 1), 1.0 / 3.0, jnp.float32)
    return lax.fori_loop(0, EG_STEPS, eg_step, (third, third, third))


def write_shares(weights, main, rem, rows, alpha_ref, ga_ref, gb_ref):
    w0, w1, w2 = weights
    lane_row = lax.broadcasted_iota(jnp.int32, (1, 128), 1)
    alpha_ref[...] = jnp.where(lane_row == 0, w0, jnp.where(lane_row == 1, w1, w2))
    lane = lax.broadcasted_iota(jnp.int32, (8, 128), 1)
    rem_task, row_task = lane // 32, (lane % 24) // 8
    gb_ref[:, 0:128] = w0 * main[0] + w1 * main[1] + w2 * main[2]
    rem = rem * jnp.where(rem_task == 0, w0, jnp.where(rem_task == 1, w1, w2))
    rem = rem + pltpu.roll(rem, 96, 1) + pltpu.roll(rem, 64, 1)
    gb_ref[:, 128:160] = rem[:, 0:32]
    rows = rows * jnp.where(row_task == 0, w0, jnp.where(row_task == 1, w1, w2))
    rows = rows + pltpu.roll(rows, 120, 1) + pltpu.roll(rows, 112, 1)
    for k in range(5):
        piece = rows if k == 0 else pltpu.roll(rows, 128 - 24 * k, 1)
        ga_ref[8 * k : 8 * k + 8, :] = piece[:, 0:8]


def exchange_kernel(n, tok_total, parts_ref, alpha_ref, ga_ref, gb_ref, recv, gram_send, gram_recv, send_sem, recv_sem, gsend_sem, grecv_sem):
    me = lax.axis_index("data")
    barrier = pltpu.get_barrier_semaphore()

    def greet(k, carry):
        pl.semaphore_signal(barrier, inc=1, device_id=(lax.rem(me + k, n),), device_id_type=MESH)
        return carry

    lax.fori_loop(1, n, greet, 0)
    pl.semaphore_wait(barrier, n - 1)

    def send(k, carry):
        dest = lax.rem(me + k, n)
        pltpu.make_async_remote_copy(
            src_ref=parts_ref.at[dest], dst_ref=recv.at[me], send_sem=send_sem, recv_sem=recv_sem,
            device_id=(dest,), device_id_type=MESH,
        ).start()
        return carry

    lax.fori_loop(1, n, send, 0)
    recv[me] = parts_ref[me]
    everyone = pltpu.make_async_remote_copy(
        src_ref=parts_ref.at[pl.ds(0, n - 1)], dst_ref=recv.at[pl.ds(0, n - 1)], send_sem=send_sem, recv_sem=recv_sem,
        device_id=(lax.rem(me + 1, n),), device_id_type=MESH,
    )
    everyone.wait_recv()
    share = jnp.sum(recv[...], axis=0) / tok_total
    main, rem, rows = (share[0], share[1], share[2]), share[3], share[4]
    gram_row = local_gram(main, rem, rows)
    gram_send[...] = gram_row
    gram_recv[me] = gram_row

    def send_gram(k, carry):
        dest = lax.rem(me + k, n)
        pltpu.make_async_remote_copy(
            src_ref=gram_send, dst_ref=gram_recv.at[me], send_sem=gsend_sem, recv_sem=grecv_sem,
            device_id=(dest,), device_id_type=MESH,
        ).start()
        return carry

    lax.fori_loop(1, n, send_gram, 0)
    every_gram = pltpu.make_async_remote_copy(
        src_ref=gram_recv.at[pl.ds(0, n - 1)], dst_ref=gram_recv.at[pl.ds(0, n - 1)], send_sem=gsend_sem, recv_sem=grecv_sem,
        device_id=(lax.rem(me + 1, n),), device_id_type=MESH,
    )
    every_gram.wait_recv()
    weights = solve_weights(jnp.sum(gram_recv[...], axis=0))
    write_shares(weights, main, rem, rows, alpha_ref, ga_ref, gb_ref)
    everyone.wait_send()
    every_gram.wait_send()


def exchange(parts, num_dev, tok_total):
    vmem = pl.BlockSpec(memory_space=pltpu.VMEM)
    return pl.pallas_call(
        functools.partial(exchange_kernel, num_dev, tok_total),
        out_shape=(
            jax.ShapeDtypeStruct((1, 128), jnp.float32),
            jax.ShapeDtypeStruct((40, 8), jnp.float32),
            jax.ShapeDtypeStruct((8, 160), jnp.float32),
        ),
        in_specs=[vmem],
        out_specs=(vmem, vmem, vmem),
        scratch_shapes=[
            pltpu.VMEM((num_dev, 5, 8, 128), jnp.float32),
            pltpu.VMEM((1, 128), jnp.float32),
            pltpu.VMEM((num_dev, 1, 128), jnp.float32),
            pltpu.SemaphoreType.DMA,
            pltpu.SemaphoreType.DMA,
            pltpu.SemaphoreType.DMA,
            pltpu.SemaphoreType.DMA,
        ],
        compiler_params=pltpu.CompilerParams(collective_id=0, has_side_effects=True),
        name="grad_exchange",
    )(parts)


def solution(mesh):
    num_dev = mesh.shape["data"]

    def device_step(tokens, labels, w_one, w_two, adapter_a, adapter_b, task_heads):
        part_a, part_b = task_grads(tokens, labels, w_one, w_two, adapter_a, adapter_b, task_heads)
        alpha, comb_a, comb_b = exchange(pack_parts(part_a, part_b, num_dev), num_dev, float(tokens.shape[0] * num_dev))
        return alpha[0, :3], comb_a, comb_b

    return jax.shard_map(device_step, mesh=mesh, in_specs=(P("data", None), P(None, "data"), P(), P(), P(), P(), P()), out_specs=(P(), P("data", None), P(None, "data")), check_vma=False)
```

```python
import functools

import jax
import jax.numpy as jnp
from jax import lax
from jax.experimental import pallas as pl
from jax.experimental.pallas import tpu as pltpu
from jax.sharding import PartitionSpec as P

EG_STEPS = 20
FWD_COLS = 512
BWD_COLS = 1280
NUM_TASKS = 3
PLANE = 8
GELU_SCALE = 0.7978845608028654
GELU_CUBE = 0.044715
MESH = pl.DeviceIdType.MESH


def full_sum(tile):
    return jnp.sum(jnp.sum(tile, axis=0, keepdims=True), axis=1, keepdims=True)


def local_gram(main, rem, rows):
    lane = lax.broadcasted_iota(jnp.int32, (8, 128), 1)
    rem_task = lane // 32
    row_task = (lane % 24) // 8
    rem_1, rem_2 = pltpu.roll(rem, 96, 1), pltpu.roll(rem, 64, 1)
    row_1, row_2 = pltpu.roll(rows, 120, 1), pltpu.roll(rows, 112, 1)

    def entry(t, s, rem_other, row_other):
        tile = main[t] * main[s]
        tile = tile + jnp.where(rem_task == t, rem * rem_other, 0.0)
        return full_sum(tile + jnp.where(row_task == t, rows * row_other, 0.0))

    entries = [entry(0, 0, rem, rows), entry(1, 1, rem, rows), entry(2, 2, rem, rows)]
    entries += [entry(0, 1, rem_1, row_1), entry(1, 2, rem_1, row_1), entry(0, 2, rem_2, row_2)]
    lane_row = lax.broadcasted_iota(jnp.int32, (1, 128), 1)
    gram_row = jnp.zeros((1, 128), jnp.float32)
    for k, value in enumerate(entries):
        gram_row = jnp.where(lane_row == k, value, gram_row)
    return gram_row


def solve_weights(gram_row):
    lane_row = lax.broadcasted_iota(jnp.int32, (1, 128), 1)
    m00, m11, m22, m01, m12, m02 = [jnp.sum(jnp.where(lane_row == k, gram_row, 0.0), axis=1, keepdims=True) for k in range(6)]
    scale = (m00 + m11 + m22) / 3.0

    def eg_step(_, w):
        w0, w1, w2 = w
        w0, w1, w2 = (
            w0 * jnp.exp(-(m00 * w0 + m01 * w1 + m02 * w2) / scale),
            w1 * jnp.exp(-(m01 * w0 + m11 * w1 + m12 * w2) / scale),
            w2 * jnp.exp(-(m02 * w0 + m12 * w1 + m22 * w2) / scale),
        )
        total = w0 + w1 + w2
        return w0 / total, w1 / total, w2 / total

    third = jnp.full((1, 1), 1.0 / 3.0, jnp.float32)
    return lax.fori_loop(0, EG_STEPS, eg_step, (third, third, third))


def write_shares(weights, main, rem, rows, alpha_ref, ga_ref, gb_ref):
    w0, w1, w2 = weights
    lane_row = lax.broadcasted_iota(jnp.int32, (1, 128), 1)
    alpha_ref[...] = jnp.where(lane_row == 0, w0, jnp.where(lane_row == 1, w1, w2))
    lane = lax.broadcasted_iota(jnp.int32, (8, 128), 1)
    rem_task, row_task = lane // 32, (lane % 24) // 8
    gb_ref[:, 0:128] = w0 * main[0] + w1 * main[1] + w2 * main[2]
    rem = rem * jnp.where(rem_task == 0, w0, jnp.where(rem_task == 1, w1, w2))
    rem = rem + pltpu.roll(rem, 96, 1) + pltpu.roll(rem, 64, 1)
    gb_ref[:, 128:160] = rem[:, 0:32]
    rows = rows * jnp.where(row_task == 0, w0, jnp.where(row_task == 1, w1, w2))
    rows = rows + pltpu.roll(rows, 120, 1) + pltpu.roll(rows, 112, 1)
    for k in range(5):
        piece = rows if k == 0 else pltpu.roll(rows, 128 - 24 * k, 1)
        ga_ref[8 * k : 8 * k + 8, :] = piece[:, 0:8]


def dot_t(lhs, rhs):
    return lax.dot_general(lhs, rhs, (((1,), (1,)), ((), ())), preferred_element_type=jnp.float32)


def dot_n(lhs, rhs):
    return jnp.dot(lhs, rhs, preferred_element_type=jnp.float32)


def gelu_and_slope(pre_act):
    square = pre_act * pre_act
    tanh = jnp.tanh(GELU_SCALE * pre_act * (1.0 + GELU_CUBE * square))
    cdf = 0.5 + 0.5 * tanh
    bell = (0.5 * GELU_SCALE) * (1.0 - tanh * tanh) * (1.0 + (3.0 * GELU_CUBE) * square)
    return pre_act * cdf, cdf + pre_act * bell


def logit_errors(logits, labels, num_classes):
    by_class = logits.T
    errors = []
    for t in range(NUM_TASKS):
        rows = by_class[16 * t : 16 * t + 16, :]
        cls = lax.broadcasted_iota(jnp.int32, rows.shape, 0)
        rows = jnp.where(cls < num_classes, rows, -jnp.inf)
        expo = jnp.exp(rows - jnp.max(rows, axis=0, keepdims=True))
        probs = expo / jnp.sum(expo, axis=0, keepdims=True)
        errors.append(probs - jnp.where(cls == labels[t : t + 1, :], 1.0, 0.0))
    errors.append(jnp.zeros((128 - 16 * NUM_TASKS, logits.shape[0]), jnp.float32))
    return jnp.concatenate(errors, axis=0).T


def pack_share_columns(main_cols, dest):
    first = 160 * dest // 128
    shift = 160 * dest - 128 * first
    main, rem = [], []
    for cols in main_cols:
        left = cols[:, 128 * first : 128 * first + 128]
        right = cols[:, 128 * first + 128 : 128 * first + 256]
        lane = lax.broadcasted_iota(jnp.int32, left.shape, 1)
        if shift == 0:
            main.append(left)
            rem.append(right)
        else:
            left, right = pltpu.roll(left, 128 - shift, 1), pltpu.roll(right, 128 - shift, 1)
            main.append(jnp.where(lane < 128 - shift, left, right))
            rem.append(right)
    lane = lax.broadcasted_iota(jnp.int32, (8, 128), 1)
    tail = jnp.where(lane < 32, rem[0], 0.0)
    tail = jnp.where(lane // 32 == 1, pltpu.roll(rem[1], 32, 1), tail)
    tail = jnp.where(lane // 32 == 2, pltpu.roll(rem[2], 64, 1), tail)
    return main, tail


def step_kernel(
    n, tok_total, num_classes,
    x_hbm, y_hbm, w1_hbm, w2_hbm, a_hbm, bm_hbm, heads_hbm,
    alpha_ref, ga_ref, gb_ref,
    x, y, w1, w2, a, bm, heads, slope, z_acc, x_t, u_t, hcat, err, dz, dp, du_t,
    send_b, recv_b, sum_b, recv_z, send_a, recv_a, gram_send, gram_recv,
    in_sem, w1_sem, w2_sem, bsend_sem, brecv_sem, zsend_sem, zrecv_sem, asend_sem, arecv_sem, gsend_sem, grecv_sem,
):
    me = lax.axis_index("data")
    plane, spot = me // PLANE, me % PLANE
    planes = n // PLANE
    d_model, d_ff = w1_hbm.shape
    toks = x_hbm.shape[0]
    fwd_steps = d_ff // FWD_COLS

    small = [
        pltpu.make_async_copy(src, dst, in_sem.at[k])
        for k, (src, dst) in enumerate([(x_hbm, x), (a_hbm, a), (bm_hbm, bm), (heads_hbm, heads), (y_hbm, y)])
    ]

    def w1_copy(j):
        return pltpu.make_async_copy(w1_hbm.at[:, pl.ds(pl.multiple_of(j * FWD_COLS, FWD_COLS), FWD_COLS)], w1.at[j], w1_sem.at[j])

    def w2_copy(j):
        rows = pl.ds(pl.multiple_of(j * FWD_COLS, FWD_COLS), FWD_COLS)
        return pltpu.make_async_copy(w2_hbm.at[rows, :], w2.at[rows, :], w2_sem.at[j])

    for copy in small:
        copy.start()

    def fetch(j, carry):
        w1_copy(j).start()
        w2_copy(j).start()
        return carry

    lax.fori_loop(0, fwd_steps, fetch, 0)

    barrier = pltpu.get_barrier_semaphore()

    def greet(k, carry):
        pl.semaphore_signal(barrier, inc=1, device_id=(lax.rem(me + k, n),), device_id_type=MESH)
        return carry

    lax.fori_loop(1, n, greet, 0)

    for copy in small:
        copy.wait()
    low_rank = dot_n(x[...], a[...])
    u_t[...] = low_rank.T.astype(jnp.bfloat16)
    low_rank = low_rank.astype(jnp.bfloat16)
    x_t[...] = x[...].astype(jnp.float32).T.astype(jnp.bfloat16)
    placed = jnp.zeros((d_model, 128), jnp.float32)
    for t in range(NUM_TASKS):
        cls = lax.broadcasted_iota(jnp.int32, (num_classes, 128), 0)
        lane = lax.broadcasted_iota(jnp.int32, (num_classes, 128), 1)
        place = jnp.where(lane == cls + 16 * t, 1.0, 0.0).astype(jnp.bfloat16)
        placed = placed + dot_n(heads[t], place)
    hcat[...] = placed.astype(jnp.bfloat16)
    z_acc[...] = jnp.zeros_like(z_acc)

    def forward(j, carry):
        cols = pl.ds(pl.multiple_of(j * FWD_COLS, FWD_COLS), FWD_COLS)
        w1_copy(j).wait()
        w2_copy(j).wait()
        pre_act = dot_n(x[...], w1[j]) + dot_n(low_rank, bm[:, cols])
        act, slope_tile = gelu_and_slope(pre_act)
        slope[:, cols] = slope_tile
        z_acc[...] += dot_n(act.astype(jnp.bfloat16), w2[cols, :])
        return carry

    lax.fori_loop(0, fwd_steps, forward, 0)

    trunk = (x[...].astype(jnp.float32) + z_acc[...]).astype(jnp.bfloat16)
    errors = logit_errors(dot_n(trunk, hcat[...]), y[...], num_classes)
    lane = lax.broadcasted_iota(jnp.int32, (toks, 128), 1)
    for t in range(NUM_TASKS):
        err[pl.ds(t * toks, toks), :] = jnp.where(lane // 16 == t, errors, 0.0).astype(jnp.bfloat16)
    dz[...] = dot_t(err[...], hcat[...]).astype(jnp.bfloat16)
    du_t[...] = jnp.zeros_like(du_t)
    pl.semaphore_wait(barrier, n - 1)

    def plane_copy(i, to):
        return pltpu.make_async_remote_copy(
            src_ref=send_b.at[i, to], dst_ref=recv_b.at[i, spot], send_sem=bsend_sem, recv_sem=brecv_sem.at[i],
            device_id=(plane * PLANE + to,), device_id_type=MESH,
        )

    def plane_wait(i):
        pltpu.make_async_remote_copy(
            src_ref=send_b.at[i, pl.ds(0, PLANE - 1)], dst_ref=recv_b.at[i, pl.ds(0, PLANE - 1)], send_sem=bsend_sem, recv_sem=brecv_sem.at[i],
            device_id=(lax.rem(me + 1, n),), device_id_type=MESH,
        ).wait_recv()

    def backward(i, carry):
        chunk = lax.rem(plane + 1 + i, planes)
        cols = pl.ds(pl.multiple_of(chunk * BWD_COLS, BWD_COLS), BWD_COLS)
        d_hidden = dot_t(dz[...], w2[cols, :])
        slope_tile = slope[:, cols]
        for t in range(NUM_TASKS):
            dp[pl.ds(t * toks, toks), :] = (d_hidden[t * toks : (t + 1) * toks, :] * slope_tile).astype(jnp.bfloat16)
        du_t[...] += dot_t(bm[:, cols], dp[...])
        grads = [dot_n(u_t[...], dp[pl.ds(t * toks, toks), :]) for t in range(NUM_TASKS)]
        for to in range(PLANE):
            main, tail = pack_share_columns(grads, to)
            for t in range(NUM_TASKS):
                send_b[i, to, t] = main[t]
            send_b[i, to, NUM_TASKS] = tail

        def send(k, carry):
            plane_copy(i, lax.rem(spot + k, PLANE)).start()
            return carry

        lax.fori_loop(1, PLANE, send, 0)
        recv_b[i, spot] = send_b[i, spot]

        @pl.when(i >= 1)
        def _():
            before = i - 1
            plane_wait(before)
            sum_b[before] = jnp.sum(recv_b[before], axis=0)
            pltpu.make_async_remote_copy(
                src_ref=sum_b.at[before], dst_ref=recv_z.at[before], send_sem=zsend_sem, recv_sem=zrecv_sem,
                device_id=(lax.rem(plane + i, planes) * PLANE + spot,), device_id_type=MESH,
            ).start()

        return carry

    lax.fori_loop(0, planes, backward, 0)

    du = du_t[...]
    du_rep = jnp.concatenate([du[:, t * toks : (t + 1) * toks] for t in range(NUM_TASKS)] * 5 + [jnp.zeros((8, toks), jnp.float32)], axis=0)
    rows_a = dot_t(x_t[...], du_rep.astype(jnp.bfloat16)).reshape(n, 5, 8, 128)
    lane = lax.broadcasted_iota(jnp.int32, (n, 8, 128), 2)
    packed = jnp.zeros((n, 8, 128), jnp.float32)
    for k in range(5):
        packed = jnp.where(lane // 24 == k, rows_a[:, k], packed)
    send_a[...] = packed

    def a_copy(to):
        return pltpu.make_async_remote_copy(
            src_ref=send_a.at[to], dst_ref=recv_a.at[me], send_sem=asend_sem, recv_sem=arecv_sem,
            device_id=(to,), device_id_type=MESH,
        )

    def send_rows(k, carry):
        a_copy(lax.rem(me + k, n)).start()
        return carry

    lax.fori_loop(1, n, send_rows, 0)
    recv_a[me] = send_a[me]

    plane_wait(planes - 1)
    every_z = pltpu.make_async_remote_copy(
        src_ref=sum_b, dst_ref=recv_z, send_sem=zsend_sem, recv_sem=zrecv_sem, device_id=(lax.rem(me + 1, n),), device_id_type=MESH
    )
    every_z.wait_recv()
    share_b = (jnp.sum(recv_b[planes - 1], axis=0) + jnp.sum(recv_z[...], axis=0)) / tok_total
    main, rem = (share_b[0], share_b[1], share_b[2]), share_b[3]
    every_a = pltpu.make_async_remote_copy(
        src_ref=send_a.at[pl.ds(0, n - 1)], dst_ref=recv_a.at[pl.ds(0, n - 1)], send_sem=asend_sem, recv_sem=arecv_sem,
        device_id=(lax.rem(me + 1, n),), device_id_type=MESH,
    )
    every_a.wait_recv()
    rows = jnp.sum(recv_a[...], axis=0) / tok_total
    gram_row = local_gram(main, rem, rows)
    gram_send[...] = gram_row
    gram_recv[me] = gram_row

    def send_gram(k, carry):
        pltpu.make_async_remote_copy(
            src_ref=gram_send, dst_ref=gram_recv.at[me], send_sem=gsend_sem, recv_sem=grecv_sem,
            device_id=(lax.rem(me + k, n),), device_id_type=MESH,
        ).start()
        return carry

    lax.fori_loop(1, n, send_gram, 0)
    every_gram = pltpu.make_async_remote_copy(
        src_ref=gram_recv.at[pl.ds(0, n - 1)], dst_ref=gram_recv.at[pl.ds(0, n - 1)], send_sem=gsend_sem, recv_sem=grecv_sem,
        device_id=(lax.rem(me + 1, n),), device_id_type=MESH,
    )
    every_gram.wait_recv()
    weights = solve_weights(jnp.sum(gram_recv[...], axis=0))
    write_shares(weights, main, rem, rows, alpha_ref, ga_ref, gb_ref)
    pltpu.make_async_remote_copy(
        src_ref=send_b.at[:, pl.ds(0, PLANE - 1)], dst_ref=recv_b.at[:, pl.ds(0, PLANE - 1)], send_sem=bsend_sem, recv_sem=brecv_sem.at[0],
        device_id=(lax.rem(me + 1, n),), device_id_type=MESH,
    ).wait_send()
    every_z.wait_send()
    every_a.wait_send()
    every_gram.wait_send()


def solution(mesh):
    num_dev = mesh.shape["data"]

    def device_step(tokens, labels, w_one, w_two, adapter_a, adapter_b, task_heads):
        toks, d_model = tokens.shape
        d_ff = w_one.shape[1]
        fwd_steps = d_ff // FWD_COLS
        planes = num_dev // PLANE
        bf16, f32 = jnp.bfloat16, jnp.float32
        dma = pltpu.SemaphoreType.DMA
        vmem = pl.BlockSpec(memory_space=pltpu.VMEM)
        hbm = pl.BlockSpec(memory_space=pltpu.HBM)
        alpha, comb_a, comb_b = pl.pallas_call(
            functools.partial(step_kernel, num_dev, float(toks * num_dev), task_heads.shape[2]),
            out_shape=(
                jax.ShapeDtypeStruct((1, 128), f32),
                jax.ShapeDtypeStruct((d_model // num_dev, 8), f32),
                jax.ShapeDtypeStruct((8, d_ff // num_dev), f32),
            ),
            in_specs=[hbm] * 7,
            out_specs=(vmem, vmem, vmem),
            scratch_shapes=[
                pltpu.VMEM(tokens.shape, bf16),
                pltpu.VMEM(labels.shape, jnp.int32),
                pltpu.VMEM((fwd_steps, d_model, FWD_COLS), bf16),
                pltpu.VMEM(w_two.shape, bf16),
                pltpu.VMEM(adapter_a.shape, bf16),
                pltpu.VMEM(adapter_b.shape, bf16),
                pltpu.VMEM(task_heads.shape, bf16),
                pltpu.VMEM((toks, d_ff), f32),
                pltpu.VMEM((toks, d_model), f32),
                pltpu.VMEM((d_model, toks), bf16),
                pltpu.VMEM((8, toks), bf16),
                pltpu.VMEM((d_model, 128), bf16),
                pltpu.VMEM((NUM_TASKS * toks, 128), bf16),
                pltpu.VMEM((NUM_TASKS * toks, d_model), bf16),
                pltpu.VMEM((NUM_TASKS * toks, BWD_COLS), bf16),
                pltpu.VMEM((8, NUM_TASKS * toks), f32),
                pltpu.VMEM((planes, PLANE, 4, 8, 128), f32),
                pltpu.VMEM((planes, PLANE, 4, 8, 128), f32),
                pltpu.VMEM((planes - 1, 4, 8, 128), f32),
                pltpu.VMEM((planes - 1, 4, 8, 128), f32),
                pltpu.VMEM((num_dev, 8, 128), f32),
                pltpu.VMEM((num_dev, 8, 128), f32),
                pltpu.VMEM((1, 128), f32),
                pltpu.VMEM((num_dev, 1, 128), f32),
                dma((5,)),
                dma((fwd_steps,)),
                dma((fwd_steps,)),
                dma,
                dma((planes,)),
                dma,
                dma,
                dma,
                dma,
                dma,
                dma,
            ],
            compiler_params=pltpu.CompilerParams(collective_id=0, has_side_effects=True, vmem_limit_bytes=60 * 1024 * 1024),
            name="grad_step",
        )(tokens, labels, w_one, w_two, adapter_a, adapter_b, task_heads)
        return alpha[0, :3], comb_a, comb_b

    return jax.shard_map(device_step, mesh=mesh, in_specs=(P("data", None), P(None, "data"), P(), P(), P(), P(), P()), out_specs=(P(), P("data", None), P(None, "data")), check_vma=False)
```

```python
import functools

import jax
import jax.numpy as jnp
from jax import lax
from jax.experimental import pallas as pl
from jax.experimental.pallas import tpu as pltpu
from jax.sharding import PartitionSpec as P

EG_STEPS = 20
FWD_COLS = 512
BWD_COLS = 1280
NUM_TASKS = 3
PLANE = 8
GELU_SCALE = 0.7978845608028654
GELU_CUBE = 0.044715
MESH = pl.DeviceIdType.MESH


def full_sum(tile):
    return jnp.sum(jnp.sum(tile, axis=0, keepdims=True), axis=1, keepdims=True)


def local_gram(main, rem, rows):
    lane = lax.broadcasted_iota(jnp.int32, (8, 128), 1)
    rem_task = lane // 32
    row_task = (lane % 24) // 8
    rem_1, rem_2 = pltpu.roll(rem, 96, 1), pltpu.roll(rem, 64, 1)
    row_1, row_2 = pltpu.roll(rows, 120, 1), pltpu.roll(rows, 112, 1)

    def entry(t, s, rem_other, row_other):
        tile = main[t] * main[s]
        tile = tile + jnp.where(rem_task == t, rem * rem_other, 0.0)
        return full_sum(tile + jnp.where(row_task == t, rows * row_other, 0.0))

    entries = [entry(0, 0, rem, rows), entry(1, 1, rem, rows), entry(2, 2, rem, rows)]
    entries += [entry(0, 1, rem_1, row_1), entry(1, 2, rem_1, row_1), entry(0, 2, rem_2, row_2)]
    lane_row = lax.broadcasted_iota(jnp.int32, (1, 128), 1)
    gram_row = jnp.zeros((1, 128), jnp.float32)
    for k, value in enumerate(entries):
        gram_row = jnp.where(lane_row == k, value, gram_row)
    return gram_row


def solve_weights(gram_row):
    lane_row = lax.broadcasted_iota(jnp.int32, (1, 128), 1)
    m00, m11, m22, m01, m12, m02 = [jnp.sum(jnp.where(lane_row == k, gram_row, 0.0), axis=1, keepdims=True) for k in range(6)]
    to_exponent = 1.4426950408889634 / ((m00 + m11 + m22) / 3.0)
    m00, m11, m22, m01, m12, m02 = [m * to_exponent for m in (m00, m11, m22, m01, m12, m02)]

    g0 = g1 = g2 = jnp.zeros((1, 1), jnp.float32)
    for step in range(EG_STEPS + 1):
        e0, e1, e2 = jnp.exp2(-g0), jnp.exp2(-g1), jnp.exp2(-g2)
        inverse = 1.0 / (e0 + e1 + e2)
        if step < EG_STEPS:
            g0 = g0 + (m00 * e0 + m01 * e1 + m02 * e2) * inverse
            g1 = g1 + (m01 * e0 + m11 * e1 + m12 * e2) * inverse
            g2 = g2 + (m02 * e0 + m12 * e1 + m22 * e2) * inverse
    return e0 * inverse, e1 * inverse, e2 * inverse


def write_shares(weights, main, rem, rows, out_ref):
    w0, w1, w2 = weights
    lane = lax.broadcasted_iota(jnp.int32, (8, 128), 1)
    rem_task, row_task = lane // 32, (lane % 24) // 8
    out_ref[0] = jnp.where(lane == 0, w0, jnp.where(lane == 1, w1, w2))
    rows = rows * jnp.where(row_task == 0, w0, jnp.where(row_task == 1, w1, w2))
    rows = rows + pltpu.roll(rows, 120, 1) + pltpu.roll(rows, 112, 1)
    out_ref[1] = rows
    out_ref[2] = w0 * main[0] + w1 * main[1] + w2 * main[2]
    rem = rem * jnp.where(rem_task == 0, w0, jnp.where(rem_task == 1, w1, w2))
    out_ref[3] = rem + pltpu.roll(rem, 96, 1) + pltpu.roll(rem, 64, 1)


def finish_kernel(tiles_ref, alpha_ref, ga_ref, gb_ref):
    alpha_ref[...] = tiles_ref[0, 0:1, 0:3]
    rows = tiles_ref[1].T
    ga_ref[...] = jnp.concatenate([rows[24 * k : 24 * k + 8, :] for k in range(5)], axis=1)
    gb_ref[:, 0:128] = tiles_ref[2]
    gb_ref[:, 128:160] = tiles_ref[3, :, 0:32]


def dot_t(lhs, rhs):
    return lax.dot_general(lhs, rhs, (((1,), (1,)), ((), ())), preferred_element_type=jnp.float32)


def dot_n(lhs, rhs):
    return jnp.dot(lhs, rhs, preferred_element_type=jnp.float32)


def gelu_and_slope(pre_act):
    square = pre_act * pre_act
    tanh = jnp.tanh(GELU_SCALE * pre_act * (1.0 + GELU_CUBE * square))
    cdf = 0.5 + 0.5 * tanh
    bell = (0.5 * GELU_SCALE) * (1.0 - tanh * tanh) * (1.0 + (3.0 * GELU_CUBE) * square)
    return pre_act * cdf, cdf + pre_act * bell


def logit_errors(logits, labels, num_classes):
    by_class = logits.T
    errors = []
    for t in range(NUM_TASKS):
        rows = by_class[16 * t : 16 * t + 16, :]
        cls = lax.broadcasted_iota(jnp.int32, rows.shape, 0)
        rows = jnp.where(cls < num_classes, rows, -jnp.inf)
        expo = jnp.exp(rows - jnp.max(rows, axis=0, keepdims=True))
        probs = expo / jnp.sum(expo, axis=0, keepdims=True)
        errors.append(probs - jnp.where(cls == labels[t : t + 1, :], 1.0, 0.0))
    errors.append(jnp.zeros((128 - 16 * NUM_TASKS, logits.shape[0]), jnp.float32))
    return jnp.concatenate(errors, axis=0).T


def pack_share_columns(main_cols, dest):
    first = 160 * dest // 128
    shift = 160 * dest - 128 * first
    main, rem = [], []
    for cols in main_cols:
        left = cols[:, 128 * first : 128 * first + 128]
        right = cols[:, 128 * first + 128 : 128 * first + 256]
        lane = lax.broadcasted_iota(jnp.int32, left.shape, 1)
        if shift == 0:
            main.append(left)
            rem.append(right)
        else:
            left, right = pltpu.roll(left, 128 - shift, 1), pltpu.roll(right, 128 - shift, 1)
            main.append(jnp.where(lane < 128 - shift, left, right))
            rem.append(right)
    lane = lax.broadcasted_iota(jnp.int32, (8, 128), 1)
    tail = jnp.where(lane < 32, rem[0], 0.0)
    tail = jnp.where(lane // 32 == 1, pltpu.roll(rem[1], 32, 1), tail)
    tail = jnp.where(lane // 32 == 2, pltpu.roll(rem[2], 64, 1), tail)
    return main, tail


def step_kernel(
    n, tok_total, num_classes,
    x_hbm, y_hbm, w1_hbm, w2_hbm, at_hbm, bm_hbm, ht_hbm,
    out_ref,
    x, y, w1, w2, at, bm, ht, slope, pre, z_acc, x_t, u_diag, bm_rep, hcat, err, dz, dp, du_acc,
    send_b, recv_b, sum_b, recv_z, send_a, recv_a, gram_send, gram_recv,
    in_sem, w1_sem, w2_sem, bsend_sem, brecv_sem, zsend_sem, zrecv_sem, asend_sem, arecv_sem, gsend_sem, grecv_sem,
):
    bf16, f32 = jnp.bfloat16, jnp.float32
    me = lax.axis_index("data")
    plane, spot = me // PLANE, me % PLANE
    planes = n // PLANE
    d_model, d_ff = w1_hbm.shape
    toks = x_hbm.shape[0]
    fwd_steps = d_ff // FWD_COLS

    small = [
        pltpu.make_async_copy(src, dst, in_sem.at[k])
        for k, (src, dst) in enumerate([(x_hbm, x), (at_hbm, at), (bm_hbm, bm), (ht_hbm, ht), (y_hbm, y)])
    ]
    def span(j):
        return pl.ds(pl.multiple_of(j * FWD_COLS, FWD_COLS), FWD_COLS)

    def w1_copy(j):
        return pltpu.make_async_copy(w1_hbm.at[:, span(j)], w1.at[:, span(j)], w1_sem.at[j])

    def w2_copy(j):
        return pltpu.make_async_copy(w2_hbm.at[span(j), :], w2.at[span(j), :], w2_sem.at[j])

    for copy in small:
        copy.start()
    w1_copy(0).start()

    def fetch(j, carry):
        w1_copy(j).start()
        w2_copy(j - 1).start()
        return carry

    lax.fori_loop(1, fwd_steps, fetch, 0)
    w2_copy(fwd_steps - 1).start()

    barrier = pltpu.get_barrier_semaphore()

    def greet(k, carry):
        pl.semaphore_signal(barrier, inc=1, device_id=(lax.rem(me + k, n),), device_id_type=MESH)
        return carry

    lax.fori_loop(1, n, greet, 0)

    for copy in small:
        copy.wait()
    low_rank = dot_t(x[...], at[...]).astype(bf16)

    def up_project(j):
        return dot_n(x[...], w1[:, span(j)]) + dot_n(low_rank, bm[:, span(j)])

    def activate(j):
        act, slope_tile = gelu_and_slope(pre[...])
        slope[:, span(j)] = slope_tile
        return act.astype(bf16)

    u_t = dot_t(at[...], x[...])
    blank = jnp.zeros_like(u_t)
    u_diag[...] = jnp.concatenate(
        [jnp.concatenate([u_t if s == t else blank for s in range(NUM_TASKS)], axis=1) for t in range(NUM_TASKS)], axis=0
    ).astype(bf16)
    bm_rep[...] = jnp.concatenate([bm[...].astype(f32)] * 16, axis=0).astype(bf16)
    gap = jnp.zeros((16 - num_classes, d_model), f32)
    heads = [part for t in range(NUM_TASKS) for part in (ht[t].astype(f32), gap)]
    hcat[...] = jnp.concatenate(heads + [jnp.zeros((128 - 16 * NUM_TASKS, d_model), f32)], axis=0).astype(bf16)
    x_t[...] = x[...].astype(f32).T.astype(bf16)

    z_acc[...] = jnp.zeros_like(z_acc)
    w1_copy(0).wait()
    pre[...] = up_project(0)

    def forward(j, carry):
        w1_copy(j + 1).wait()
        w2_copy(j).wait()
        act = activate(j)
        pre[...] = up_project(j + 1)
        z_acc[...] += dot_n(act, w2[span(j), :])
        return carry

    lax.fori_loop(0, fwd_steps - 1, forward, 0)
    w2_copy(fwd_steps - 1).wait()
    z_acc[...] += dot_n(activate(fwd_steps - 1), w2[span(fwd_steps - 1), :])

    trunk = (x[...].astype(f32) + z_acc[...]).astype(bf16)
    errors = logit_errors(dot_t(trunk, hcat[...]), y[...], num_classes)
    lane = lax.broadcasted_iota(jnp.int32, (toks, 128), 1)
    for t in range(NUM_TASKS):
        err[pl.ds(t * toks, toks), :] = jnp.where(lane // 16 == t, errors, 0.0).astype(bf16)
    dz[...] = dot_n(err[...], hcat[...]).astype(bf16)
    pl.semaphore_wait(barrier, n - 1)
    SEND_ON = True

    def plane_send(i):
        if not SEND_ON:
            return

        def send(k, carry):
            to = lax.rem(spot + k, PLANE)
            pltpu.make_async_remote_copy(
                src_ref=send_b.at[i, to], dst_ref=recv_b.at[i, spot], send_sem=bsend_sem, recv_sem=brecv_sem.at[i],
                device_id=(plane * PLANE + to,), device_id_type=MESH,
            ).start()
            return carry

        lax.fori_loop(1, PLANE, send, 0)
        recv_b[i, spot] = send_b[i, spot]

    def plane_wait(i):
        pltpu.make_async_remote_copy(
            src_ref=send_b.at[i, pl.ds(0, PLANE - 1)], dst_ref=recv_b.at[i, pl.ds(0, PLANE - 1)], send_sem=bsend_sem, recv_sem=brecv_sem.at[i],
            device_id=(lax.rem(me + 1, n),), device_id_type=MESH,
        ).wait_recv()

    def across_send(i):
        if not SEND_ON:
            return
        plane_wait(i)
        sum_b[i] = jnp.sum(recv_b[i], axis=0)
        pltpu.make_async_remote_copy(
            src_ref=sum_b.at[i], dst_ref=recv_z.at[i], send_sem=zsend_sem, recv_sem=zrecv_sem,
            device_id=(lax.rem(plane + 1 + i, planes) * PLANE + spot,), device_id_type=MESH,
        ).start()

    def chunk_cols(i):
        chunk = lax.rem(plane + 1 + i, planes)
        return pl.ds(pl.multiple_of(chunk * BWD_COLS, BWD_COLS), BWD_COLS)

    def back_project(i):
        cols = chunk_cols(i)
        d_hidden = dot_t(dz[...], w2[cols, :])
        slope_tile = slope[:, cols]
        for t in range(NUM_TASKS):
            dp[pl.ds(t * toks, toks), :] = (d_hidden[t * toks : (t + 1) * toks, :] * slope_tile).astype(bf16)

    def low_rank_grad(i):
        du_acc[...] += dot_t(dp[...], bm_rep[:, chunk_cols(i)])

    def adapter_grad(i):
        grads = dot_n(u_diag[...], dp[...])
        for to in range(PLANE):
            main, tail = pack_share_columns([grads[8 * t : 8 * t + 8, :] for t in range(NUM_TASKS)], to)
            for t in range(NUM_TASKS):
                send_b[i, to, t] = main[t]
            send_b[i, to, NUM_TASKS] = tail

    du_acc[...] = jnp.zeros_like(du_acc)

    def backward(i, carry):
        back_project(i)
        low_rank_grad(i)
        adapter_grad(i)
        plane_send(i)

        @pl.when(i >= 1)
        def _():
            across_send(i - 1)

        return carry

    lax.fori_loop(0, planes, backward, 0)

    lane = lax.broadcasted_iota(jnp.int32, (toks, 128), 1)
    du = du_acc[2 * toks :, :]
    for t in range(NUM_TASKS - 1):
        du = jnp.where((lane // 8) % NUM_TASKS == t, du_acc[t * toks : (t + 1) * toks, :], du)
    rows_a = dot_n(x_t[...], du.astype(bf16)).reshape(n, 5, 8, 128)
    lane = lax.broadcasted_iota(jnp.int32, (n, 8, 128), 2)
    packed = jnp.where(lane < 120, rows_a[:, 4], 0.0)
    for k in range(4):
        packed = jnp.where(lane // 24 == k, rows_a[:, k], packed)
    send_a[...] = packed

    def send_rows(k, carry):
        to = lax.rem(me + k, n)
        pltpu.make_async_remote_copy(
            src_ref=send_a.at[to], dst_ref=recv_a.at[me], send_sem=asend_sem, recv_sem=arecv_sem,
            device_id=(to,), device_id_type=MESH,
        ).start()
        return carry

    lax.fori_loop(PLANE, n, send_rows, 0)
    lax.fori_loop(1, PLANE, send_rows, 0)
    recv_a[me] = send_a[me]

    plane_wait(planes - 1)
    every_z = pltpu.make_async_remote_copy(
        src_ref=sum_b, dst_ref=recv_z, send_sem=zsend_sem, recv_sem=zrecv_sem, device_id=(lax.rem(me + 1, n),), device_id_type=MESH
    )
    every_z.wait_recv()
    share_b = (jnp.sum(recv_b[planes - 1], axis=0) + jnp.sum(recv_z[...], axis=0)) / tok_total
    main, rem = (share_b[0], share_b[1], share_b[2]), share_b[3]
    every_a = pltpu.make_async_remote_copy(
        src_ref=send_a.at[pl.ds(0, n - 1)], dst_ref=recv_a.at[pl.ds(0, n - 1)], send_sem=asend_sem, recv_sem=arecv_sem,
        device_id=(lax.rem(me + 1, n),), device_id_type=MESH,
    )
    every_a.wait_recv()
    rows = jnp.sum(recv_a[...], axis=0) / tok_total
    gram_row = local_gram(main, rem, rows)
    gram_send[...] = gram_row
    gram_recv[me] = gram_row

    def send_gram(k, carry):
        pltpu.make_async_remote_copy(
            src_ref=gram_send, dst_ref=gram_recv.at[me], send_sem=gsend_sem, recv_sem=grecv_sem,
            device_id=(lax.rem(me + k, n),), device_id_type=MESH,
        ).start()
        return carry

    lax.fori_loop(PLANE, n, send_gram, 0)
    lax.fori_loop(1, PLANE, send_gram, 0)
    every_gram = pltpu.make_async_remote_copy(
        src_ref=gram_recv.at[pl.ds(0, n - 1)], dst_ref=gram_recv.at[pl.ds(0, n - 1)], send_sem=gsend_sem, recv_sem=grecv_sem,
        device_id=(lax.rem(me + 1, n),), device_id_type=MESH,
    )
    pltpu.make_async_remote_copy(
        src_ref=send_b.at[:, pl.ds(0, PLANE - 1)], dst_ref=recv_b.at[:, pl.ds(0, PLANE - 1)], send_sem=bsend_sem, recv_sem=brecv_sem.at[0],
        device_id=(lax.rem(me + 1, n),), device_id_type=MESH,
    ).wait_send()
    every_z.wait_send()
    every_a.wait_send()
    every_gram.wait_recv()
    weights = solve_weights(jnp.sum(gram_recv[...], axis=0))
    write_shares(weights, main, rem, rows, out_ref)
    every_gram.wait_send()


def solution(mesh):
    num_dev = mesh.shape["data"]

    def device_step(tokens, labels, w_one, w_two, adapter_a, adapter_b, task_heads):
        toks, d_model = tokens.shape
        d_ff = w_one.shape[1]
        planes = num_dev // PLANE
        fwd_steps = d_ff // FWD_COLS
        bf16, f32 = jnp.bfloat16, jnp.float32
        dma = pltpu.SemaphoreType.DMA
        vmem = pl.BlockSpec(memory_space=pltpu.VMEM)
        hbm = pl.BlockSpec(memory_space=pltpu.HBM)
        adapter_t = adapter_a.T
        heads_t = task_heads.transpose(0, 2, 1)
        tiles = pl.pallas_call(
            functools.partial(step_kernel, num_dev, float(toks * num_dev), task_heads.shape[2]),
            out_shape=jax.ShapeDtypeStruct((4, 8, 128), f32),
            in_specs=[hbm] * 7,
            out_specs=vmem,
            scratch_shapes=[
                pltpu.VMEM(tokens.shape, bf16),
                pltpu.VMEM(labels.shape, jnp.int32),
                pltpu.VMEM(w_one.shape, bf16),
                pltpu.VMEM(w_two.shape, bf16),
                pltpu.VMEM(adapter_t.shape, bf16),
                pltpu.VMEM(adapter_b.shape, bf16),
                pltpu.VMEM(heads_t.shape, bf16),
                pltpu.VMEM((toks, d_ff), f32),
                pltpu.VMEM((toks, FWD_COLS), f32),
                pltpu.VMEM((toks, d_model), f32),
                pltpu.VMEM((d_model, toks), bf16),
                pltpu.VMEM((8 * NUM_TASKS, NUM_TASKS * toks), bf16),
                pltpu.VMEM((128, d_ff), bf16),
                pltpu.VMEM((128, d_model), bf16),
                pltpu.VMEM((NUM_TASKS * toks, 128), bf16),
                pltpu.VMEM((NUM_TASKS * toks, d_model), bf16),
                pltpu.VMEM((NUM_TASKS * toks, BWD_COLS), bf16),
                pltpu.VMEM((NUM_TASKS * toks, 128), f32),
                pltpu.VMEM((planes, PLANE, 4, 8, 128), f32),
                pltpu.VMEM((planes, PLANE, 4, 8, 128), f32),
                pltpu.VMEM((planes - 1, 4, 8, 128), f32),
                pltpu.VMEM((planes - 1, 4, 8, 128), f32),
                pltpu.VMEM((num_dev, 8, 128), f32),
                pltpu.VMEM((num_dev, 8, 128), f32),
                pltpu.VMEM((1, 128), f32),
                pltpu.VMEM((num_dev, 1, 128), f32),
                dma((5,)),
                dma((fwd_steps,)),
                dma((fwd_steps,)),
                dma,
                dma((planes,)),
                dma,
                dma,
                dma,
                dma,
                dma,
                dma,
            ],
            compiler_params=pltpu.CompilerParams(collective_id=0, has_side_effects=True, vmem_limit_bytes=60 * 1024 * 1024),
            name="grad_step",
        )(tokens, labels, w_one, w_two, adapter_t, adapter_b, heads_t)
        alpha, comb_at, comb_b = pl.pallas_call(
            finish_kernel,
            out_shape=(
                jax.ShapeDtypeStruct((1, NUM_TASKS), f32),
                jax.ShapeDtypeStruct((8, d_model // num_dev), f32),
                jax.ShapeDtypeStruct((8, d_ff // num_dev), f32),
            ),
            in_specs=[vmem],
            out_specs=(vmem, vmem, vmem),
            name="write_out",
        )(tiles)
        return alpha[0], comb_at.T, comb_b

    return jax.shard_map(device_step, mesh=mesh, in_specs=(P("data", None), P(None, "data"), P(), P(), P(), P(), P()), out_specs=(P(), P("data", None), P(None, "data")), check_vma=False)
```

```python
import functools

import jax
import jax.numpy as jnp
from jax import lax
from jax.experimental import pallas as pl
from jax.experimental.pallas import tpu as pltpu
from jax.sharding import PartitionSpec as P

EG_STEPS = 20
FWD_COLS = 512
BWD_COLS = 1280
NUM_TASKS = 3
PLANE = 8
GELU_SCALE = 0.7978845608028654
GELU_CUBE = 0.044715
MESH = pl.DeviceIdType.MESH


def full_sum(tile):
    return jnp.sum(jnp.sum(tile, axis=0, keepdims=True), axis=1, keepdims=True)


def local_gram(main, rem, rows):
    lane = lax.broadcasted_iota(jnp.int32, (8, 128), 1)
    rem_task = lane // 32
    row_task = (lane % 24) // 8
    rem_1, rem_2 = pltpu.roll(rem, 96, 1), pltpu.roll(rem, 64, 1)
    row_1, row_2 = pltpu.roll(rows, 120, 1), pltpu.roll(rows, 112, 1)

    def entry(t, s, rem_other, row_other):
        tile = main[t] * main[s]
        tile = tile + jnp.where(rem_task == t, rem * rem_other, 0.0)
        return full_sum(tile + jnp.where(row_task == t, rows * row_other, 0.0))

    entries = [entry(0, 0, rem, rows), entry(1, 1, rem, rows), entry(2, 2, rem, rows)]
    entries += [entry(0, 1, rem_1, row_1), entry(1, 2, rem_1, row_1), entry(0, 2, rem_2, row_2)]
    lane_row = lax.broadcasted_iota(jnp.int32, (1, 128), 1)
    gram_row = jnp.zeros((1, 128), jnp.float32)
    for k, value in enumerate(entries):
        gram_row = jnp.where(lane_row == k, value, gram_row)
    return gram_row


def solve_weights(gram_row):
    lane_row = lax.broadcasted_iota(jnp.int32, (1, 128), 1)
    m00, m11, m22, m01, m12, m02 = [jnp.sum(jnp.where(lane_row == k, gram_row, 0.0), axis=1, keepdims=True) for k in range(6)]
    to_exponent = 1.4426950408889634 / ((m00 + m11 + m22) / 3.0)
    m00, m11, m22, m01, m12, m02 = [m * to_exponent for m in (m00, m11, m22, m01, m12, m02)]

    g0 = g1 = g2 = jnp.zeros((1, 1), jnp.float32)
    for step in range(EG_STEPS + 1):
        e0, e1, e2 = jnp.exp2(-g0), jnp.exp2(-g1), jnp.exp2(-g2)
        inverse = 1.0 / (e0 + e1 + e2)
        if step < EG_STEPS:
            g0 = g0 + (m00 * e0 + m01 * e1 + m02 * e2) * inverse
            g1 = g1 + (m01 * e0 + m11 * e1 + m12 * e2) * inverse
            g2 = g2 + (m02 * e0 + m12 * e1 + m22 * e2) * inverse
    return e0 * inverse, e1 * inverse, e2 * inverse


def write_shares(weights, main, rem, rows, out_ref):
    w0, w1, w2 = weights
    lane = lax.broadcasted_iota(jnp.int32, (8, 128), 1)
    rem_task, row_task = lane // 32, (lane % 24) // 8
    out_ref[0] = jnp.where(lane == 0, w0, jnp.where(lane == 1, w1, w2))
    rows = rows * jnp.where(row_task == 0, w0, jnp.where(row_task == 1, w1, w2))
    rows = rows + pltpu.roll(rows, 120, 1) + pltpu.roll(rows, 112, 1)
    out_ref[1] = rows
    out_ref[2] = w0 * main[0] + w1 * main[1] + w2 * main[2]
    rem = rem * jnp.where(rem_task == 0, w0, jnp.where(rem_task == 1, w1, w2))
    out_ref[3] = rem + pltpu.roll(rem, 96, 1) + pltpu.roll(rem, 64, 1)


def finish_kernel(tiles_ref, alpha_ref, ga_ref, gb_ref):
    alpha_ref[...] = tiles_ref[0, 0:1, 0:3]
    rows = tiles_ref[1].T
    ga_ref[...] = jnp.concatenate([rows[24 * k : 24 * k + 8, :] for k in range(5)], axis=1)
    gb_ref[:, 0:128] = tiles_ref[2]
    gb_ref[:, 128:160] = tiles_ref[3, :, 0:32]


def dot_t(lhs, rhs):
    return lax.dot_general(lhs, rhs, (((1,), (1,)), ((), ())), preferred_element_type=jnp.float32)


def dot_n(lhs, rhs):
    return jnp.dot(lhs, rhs, preferred_element_type=jnp.float32)


def gelu_and_slope(pre_act):
    square = pre_act * pre_act
    tanh = jnp.tanh(GELU_SCALE * pre_act * (1.0 + GELU_CUBE * square))
    cdf = 0.5 + 0.5 * tanh
    bell = (0.5 * GELU_SCALE) * (1.0 - tanh * tanh) * (1.0 + (3.0 * GELU_CUBE) * square)
    return pre_act * cdf, cdf + pre_act * bell


def logit_errors(logits, labels, num_classes):
    by_class = logits.T
    errors = []
    for t in range(NUM_TASKS):
        rows = by_class[16 * t : 16 * t + 16, :]
        cls = lax.broadcasted_iota(jnp.int32, rows.shape, 0)
        rows = jnp.where(cls < num_classes, rows, -jnp.inf)
        expo = jnp.exp(rows - jnp.max(rows, axis=0, keepdims=True))
        probs = expo / jnp.sum(expo, axis=0, keepdims=True)
        errors.append(probs - jnp.where(cls == labels[t : t + 1, :], 1.0, 0.0))
    errors.append(jnp.zeros((128 - 16 * NUM_TASKS, logits.shape[0]), jnp.float32))
    return jnp.concatenate(errors, axis=0).T


def pack_share_columns(main_cols, dest):
    first = 160 * dest // 128
    shift = 160 * dest - 128 * first
    main, rem = [], []
    for cols in main_cols:
        left = cols[:, 128 * first : 128 * first + 128]
        right = cols[:, 128 * first + 128 : 128 * first + 256]
        lane = lax.broadcasted_iota(jnp.int32, left.shape, 1)
        if shift == 0:
            main.append(left)
            rem.append(right)
        else:
            left, right = pltpu.roll(left, 128 - shift, 1), pltpu.roll(right, 128 - shift, 1)
            main.append(jnp.where(lane < 128 - shift, left, right))
            rem.append(right)
    lane = lax.broadcasted_iota(jnp.int32, (8, 128), 1)
    tail = jnp.where(lane < 32, rem[0], 0.0)
    tail = jnp.where(lane // 32 == 1, pltpu.roll(rem[1], 32, 1), tail)
    tail = jnp.where(lane // 32 == 2, pltpu.roll(rem[2], 64, 1), tail)
    return main, tail


def step_kernel(
    n, tok_total, num_classes,
    x_hbm, y_hbm, w1_hbm, w2_hbm, at_hbm, bm_hbm, ht_hbm,
    out_ref,
    x, y, w1, w2, at, bm, ht, slope, pre, z_acc, x_t, u_diag, bm_rep, hcat, err, dz, dp, du_acc,
    send_b, recv_b, sum_b, recv_z, send_a, recv_a, gram_send, gram_recv,
    in_sem, w1_sem, w2_sem, bsend_sem, brecv_sem, zsend_sem, zrecv_sem, asend_sem, arecv_sem, gsend_sem, grecv_sem,
):
    bf16, f32 = jnp.bfloat16, jnp.float32
    me = lax.axis_index("data")
    plane, spot = me // PLANE, me % PLANE
    planes = n // PLANE
    d_model, d_ff = w1_hbm.shape
    toks = x_hbm.shape[0]
    fwd_steps = d_ff // FWD_COLS

    small = [
        pltpu.make_async_copy(src, dst, in_sem.at[k])
        for k, (src, dst) in enumerate([(x_hbm, x), (at_hbm, at), (bm_hbm, bm), (ht_hbm, ht), (y_hbm, y)])
    ]
    def span(j):
        return pl.ds(pl.multiple_of(j * FWD_COLS, FWD_COLS), FWD_COLS)

    def w1_copy(j):
        return pltpu.make_async_copy(w1_hbm.at[:, span(j)], w1.at[:, span(j)], w1_sem.at[j])

    def w2_copy(j):
        return pltpu.make_async_copy(w2_hbm.at[span(j), :], w2.at[span(j), :], w2_sem.at[j])

    for copy in small:
        copy.start()
    w1_copy(0).start()

    def fetch(j, carry):
        w1_copy(j).start()
        w2_copy(j - 1).start()
        return carry

    lax.fori_loop(1, fwd_steps, fetch, 0)
    w2_copy(fwd_steps - 1).start()

    barrier = pltpu.get_barrier_semaphore()

    def greet(k, carry):
        pl.semaphore_signal(barrier, inc=1, device_id=(lax.rem(me + k, n),), device_id_type=MESH)
        return carry

    lax.fori_loop(1, n, greet, 0)

    for copy in small:
        copy.wait()
    low_rank = dot_t(x[...], at[...]).astype(bf16)

    def up_project(j):
        return dot_n(x[...], w1[:, span(j)]) + dot_n(low_rank, bm[:, span(j)])

    def activate(j):
        act, slope_tile = gelu_and_slope(pre[...])
        slope[:, span(j)] = slope_tile
        return act.astype(bf16)

    u_t = dot_t(at[...], x[...])
    blank = jnp.zeros_like(u_t)
    u_diag[...] = jnp.concatenate(
        [jnp.concatenate([u_t if s == t else blank for s in range(NUM_TASKS)], axis=1) for t in range(NUM_TASKS)], axis=0
    ).astype(bf16)
    bm_rep[...] = jnp.concatenate([bm[...].astype(f32)] * 16, axis=0).astype(bf16)
    gap = jnp.zeros((16 - num_classes, d_model), f32)
    heads = [part for t in range(NUM_TASKS) for part in (ht[t].astype(f32), gap)]
    hcat[...] = jnp.concatenate(heads + [jnp.zeros((128 - 16 * NUM_TASKS, d_model), f32)], axis=0).astype(bf16)
    x_t[...] = x[...].astype(f32).T.astype(bf16)

    z_acc[...] = jnp.zeros_like(z_acc)
    w1_copy(0).wait()
    pre[...] = up_project(0)

    def forward(j, carry):
        w1_copy(j + 1).wait()
        w2_copy(j).wait()
        act = activate(j)
        pre[...] = up_project(j + 1)
        z_acc[...] += dot_n(act, w2[span(j), :])
        return carry

    lax.fori_loop(0, fwd_steps - 1, forward, 0)
    w2_copy(fwd_steps - 1).wait()
    z_acc[...] += dot_n(activate(fwd_steps - 1), w2[span(fwd_steps - 1), :])

    trunk = (x[...].astype(f32) + z_acc[...]).astype(bf16)
    errors = logit_errors(dot_t(trunk, hcat[...]), y[...], num_classes)
    lane = lax.broadcasted_iota(jnp.int32, (toks, 128), 1)
    for t in range(NUM_TASKS):
        err[pl.ds(t * toks, toks), :] = jnp.where(lane // 16 == t, errors, 0.0).astype(bf16)
    dz[...] = dot_n(err[...], hcat[...]).astype(bf16)
    pl.semaphore_wait(barrier, n - 1)
    SEND_ON = True

    def plane_send(i):
        if not SEND_ON:
            return

        def send(k, carry):
            to = lax.rem(spot + k, PLANE)
            pltpu.make_async_remote_copy(
                src_ref=send_b.at[i, to], dst_ref=recv_b.at[i, spot], send_sem=bsend_sem, recv_sem=brecv_sem.at[i],
                device_id=(plane * PLANE + to,), device_id_type=MESH,
            ).start()
            return carry

        lax.fori_loop(1, PLANE, send, 0)
        recv_b[i, spot] = send_b[i, spot]

    def plane_wait(i):
        pltpu.make_async_remote_copy(
            src_ref=send_b.at[i, pl.ds(0, PLANE - 1)], dst_ref=recv_b.at[i, pl.ds(0, PLANE - 1)], send_sem=bsend_sem, recv_sem=brecv_sem.at[i],
            device_id=(lax.rem(me + 1, n),), device_id_type=MESH,
        ).wait_recv()

    def across_send(i):
        if not SEND_ON:
            return
        plane_wait(i)
        sum_b[i] = jnp.sum(recv_b[i], axis=0)
        pltpu.make_async_remote_copy(
            src_ref=sum_b.at[i], dst_ref=recv_z.at[i], send_sem=zsend_sem, recv_sem=zrecv_sem,
            device_id=(lax.rem(plane + 1 + i, planes) * PLANE + spot,), device_id_type=MESH,
        ).start()

    def chunk_cols(i):
        chunk = lax.rem(plane + 1 + i, planes)
        return pl.ds(pl.multiple_of(chunk * BWD_COLS, BWD_COLS), BWD_COLS)

    def back_project(i):
        cols = chunk_cols(i)
        d_hidden = dot_t(dz[...], w2[cols, :])
        slope_tile = slope[:, cols]
        for t in range(NUM_TASKS):
            dp[pl.ds(t * toks, toks), :] = (d_hidden[t * toks : (t + 1) * toks, :] * slope_tile).astype(bf16)

    def low_rank_grad(i):
        du_acc[...] += dot_t(dp[...], bm_rep[:, chunk_cols(i)])

    def adapter_grad(i):
        grads = dot_n(u_diag[...], dp[...])
        for to in range(PLANE):
            main, tail = pack_share_columns([grads[8 * t : 8 * t + 8, :] for t in range(NUM_TASKS)], to)
            for t in range(NUM_TASKS):
                send_b[i, to, t] = main[t]
            send_b[i, to, NUM_TASKS] = tail

    du_acc[...] = jnp.zeros_like(du_acc)

    def backward(i, carry):
        back_project(i)
        low_rank_grad(i)
        adapter_grad(i)
        plane_send(i)

        @pl.when(i >= 1)
        def _():
            across_send(i - 1)

        return carry

    lax.fori_loop(0, planes, backward, 0)

    lane = lax.broadcasted_iota(jnp.int32, (toks, 128), 1)
    du = du_acc[2 * toks :, :]
    for t in range(NUM_TASKS - 1):
        du = jnp.where((lane // 8) % NUM_TASKS == t, du_acc[t * toks : (t + 1) * toks, :], du)
    rows_a = dot_n(x_t[...], du.astype(bf16)).reshape(n, 5, 8, 128)
    lane = lax.broadcasted_iota(jnp.int32, (n, 8, 128), 2)
    packed = jnp.where(lane < 120, rows_a[:, 4], 0.0)
    for k in range(4):
        packed = jnp.where(lane // 24 == k, rows_a[:, k], packed)
    send_a[...] = packed

    def send_rows(k, carry):
        to = lax.rem(me + k, n)
        pltpu.make_async_remote_copy(
            src_ref=send_a.at[to], dst_ref=recv_a.at[me], send_sem=asend_sem, recv_sem=arecv_sem,
            device_id=(to,), device_id_type=MESH,
        ).start()
        return carry

    lax.fori_loop(PLANE, n, send_rows, 0)
    lax.fori_loop(1, PLANE, send_rows, 0)
    recv_a[me] = send_a[me]

    plane_wait(planes - 1)
    every_z = pltpu.make_async_remote_copy(
        src_ref=sum_b, dst_ref=recv_z, send_sem=zsend_sem, recv_sem=zrecv_sem, device_id=(lax.rem(me + 1, n),), device_id_type=MESH
    )
    every_z.wait_recv()
    share_b = (jnp.sum(recv_b[planes - 1], axis=0) + jnp.sum(recv_z[...], axis=0)) / tok_total
    main, rem = (share_b[0], share_b[1], share_b[2]), share_b[3]
    every_a = pltpu.make_async_remote_copy(
        src_ref=send_a.at[pl.ds(0, n - 1)], dst_ref=recv_a.at[pl.ds(0, n - 1)], send_sem=asend_sem, recv_sem=arecv_sem,
        device_id=(lax.rem(me + 1, n),), device_id_type=MESH,
    )
    every_a.wait_recv()
    rows = jnp.sum(recv_a[...], axis=0) / tok_total
    gram_row = local_gram(main, rem, rows)
    gram_send[...] = gram_row
    gram_recv[me] = gram_row

    def send_gram(k, carry):
        pltpu.make_async_remote_copy(
            src_ref=gram_send, dst_ref=gram_recv.at[me], send_sem=gsend_sem, recv_sem=grecv_sem,
            device_id=(lax.rem(me + k, n),), device_id_type=MESH,
        ).start()
        return carry

    lax.fori_loop(PLANE, n, send_gram, 0)
    lax.fori_loop(1, PLANE, send_gram, 0)
    every_gram = pltpu.make_async_remote_copy(
        src_ref=gram_recv.at[pl.ds(0, n - 1)], dst_ref=gram_recv.at[pl.ds(0, n - 1)], send_sem=gsend_sem, recv_sem=grecv_sem,
        device_id=(lax.rem(me + 1, n),), device_id_type=MESH,
    )
    pltpu.make_async_remote_copy(
        src_ref=send_b.at[:, pl.ds(0, PLANE - 1)], dst_ref=recv_b.at[:, pl.ds(0, PLANE - 1)], send_sem=bsend_sem, recv_sem=brecv_sem.at[0],
        device_id=(lax.rem(me + 1, n),), device_id_type=MESH,
    ).wait_send()
    every_z.wait_send()
    every_a.wait_send()
    every_gram.wait_recv()
    weights = solve_weights(jnp.sum(gram_recv[...], axis=0))
    write_shares(weights, main, rem, rows, out_ref)
    every_gram.wait_send()


def solution(mesh):
    num_dev = mesh.shape["data"]

    def device_step(tokens, labels, w_one, w_two, adapter_a, adapter_b, task_heads):
        toks, d_model = tokens.shape
        d_ff = w_one.shape[1]
        planes = num_dev // PLANE
        fwd_steps = d_ff // FWD_COLS
        bf16, f32 = jnp.bfloat16, jnp.float32
        dma = pltpu.SemaphoreType.DMA
        vmem = pl.BlockSpec(memory_space=pltpu.VMEM)
        hbm = pl.BlockSpec(memory_space=pltpu.HBM)
        adapter_t = adapter_a.T
        heads_t = task_heads.transpose(0, 2, 1)
        tiles = pl.pallas_call(
            functools.partial(step_kernel, num_dev, float(toks * num_dev), task_heads.shape[2]),
            out_shape=jax.ShapeDtypeStruct((4, 8, 128), f32),
            in_specs=[hbm] * 7,
            out_specs=vmem,
            scratch_shapes=[
                pltpu.VMEM(tokens.shape, bf16),
                pltpu.VMEM(labels.shape, jnp.int32),
                pltpu.VMEM(w_one.shape, bf16),
                pltpu.VMEM(w_two.shape, bf16),
                pltpu.VMEM(adapter_t.shape, bf16),
                pltpu.VMEM(adapter_b.shape, bf16),
                pltpu.VMEM(heads_t.shape, bf16),
                pltpu.VMEM((toks, d_ff), f32),
                pltpu.VMEM((toks, FWD_COLS), f32),
                pltpu.VMEM((toks, d_model), f32),
                pltpu.VMEM((d_model, toks), bf16),
                pltpu.VMEM((8 * NUM_TASKS, NUM_TASKS * toks), bf16),
                pltpu.VMEM((128, d_ff), bf16),
                pltpu.VMEM((128, d_model), bf16),
                pltpu.VMEM((NUM_TASKS * toks, 128), bf16),
                pltpu.VMEM((NUM_TASKS * toks, d_model), bf16),
                pltpu.VMEM((NUM_TASKS * toks, BWD_COLS), bf16),
                pltpu.VMEM((NUM_TASKS * toks, 128), f32),
                pltpu.VMEM((planes, PLANE, 4, 8, 128), f32),
                pltpu.VMEM((planes, PLANE, 4, 8, 128), f32),
                pltpu.VMEM((planes - 1, 4, 8, 128), f32),
                pltpu.VMEM((planes - 1, 4, 8, 128), f32),
                pltpu.VMEM((num_dev, 8, 128), f32),
                pltpu.VMEM((num_dev, 8, 128), f32),
                pltpu.VMEM((1, 128), f32),
                pltpu.VMEM((num_dev, 1, 128), f32),
                dma((5,)),
                dma((fwd_steps,)),
                dma((fwd_steps,)),
                dma,
                dma((planes,)),
                dma,
                dma,
                dma,
                dma,
                dma,
                dma,
            ],
            compiler_params=pltpu.CompilerParams(collective_id=0, has_side_effects=True, vmem_limit_bytes=52 * 1024 * 1024),
            name="grad_step",
        )(*[pltpu.with_memory_space_constraint(arg, pltpu.HBM) for arg in (tokens, labels, w_one, w_two, adapter_t, adapter_b, heads_t)])
        alpha, comb_at, comb_b = pl.pallas_call(
            finish_kernel,
            out_shape=(
                jax.ShapeDtypeStruct((1, NUM_TASKS), f32),
                jax.ShapeDtypeStruct((8, d_model // num_dev), f32),
                jax.ShapeDtypeStruct((8, d_ff // num_dev), f32),
            ),
            in_specs=[vmem],
            out_specs=(vmem, vmem, vmem),
            compiler_params=pltpu.CompilerParams(vmem_limit_bytes=1024 * 1024),
            name="write_out",
        )(tiles)
        return alpha[0], comb_at.T, comb_b

    return jax.shard_map(device_step, mesh=mesh, in_specs=(P("data", None), P(None, "data"), P(), P(), P(), P(), P()), out_specs=(P(), P("data", None), P(None, "data")), check_vma=False)
```

```python
import functools

import jax
import jax.numpy as jnp
from jax import lax
from jax.experimental import pallas as pl
from jax.experimental.pallas import tpu as pltpu
from jax.sharding import PartitionSpec as P

EG_STEPS = 20
FWD_COLS = 512
BWD_COLS = 1280
NUM_TASKS = 3
PLANE = 8
GELU_SCALE = 0.7978845608028654
GELU_CUBE = 0.044715
MESH = pl.DeviceIdType.MESH


def full_sum(tile):
    return jnp.sum(jnp.sum(tile, axis=0, keepdims=True), axis=1, keepdims=True)


def local_gram(main, rem, rows):
    lane = lax.broadcasted_iota(jnp.int32, (8, 128), 1)
    rem_task = lane // 32
    row_task = (lane % 24) // 8
    rem_1, rem_2 = pltpu.roll(rem, 96, 1), pltpu.roll(rem, 64, 1)
    row_1, row_2 = pltpu.roll(rows, 120, 1), pltpu.roll(rows, 112, 1)

    def entry(t, s, rem_other, row_other):
        tile = main[t] * main[s]
        tile = tile + jnp.where(rem_task == t, rem * rem_other, 0.0)
        return full_sum(tile + jnp.where(row_task == t, rows * row_other, 0.0))

    entries = [entry(0, 0, rem, rows), entry(1, 1, rem, rows), entry(2, 2, rem, rows)]
    entries += [entry(0, 1, rem_1, row_1), entry(1, 2, rem_1, row_1), entry(0, 2, rem_2, row_2)]
    lane_row = lax.broadcasted_iota(jnp.int32, (1, 128), 1)
    gram_row = jnp.zeros((1, 128), jnp.float32)
    for k, value in enumerate(entries):
        gram_row = jnp.where(lane_row == k, value, gram_row)
    return gram_row


def solve_weights(gram_row):
    lane_row = lax.broadcasted_iota(jnp.int32, (1, 128), 1)
    m00, m11, m22, m01, m12, m02 = [jnp.sum(jnp.where(lane_row == k, gram_row, 0.0), axis=1, keepdims=True) for k in range(6)]
    to_exponent = 1.4426950408889634 / ((m00 + m11 + m22) / 3.0)
    m00, m11, m22, m01, m12, m02 = [m * to_exponent for m in (m00, m11, m22, m01, m12, m02)]

    g0 = g1 = g2 = jnp.zeros((1, 1), jnp.float32)
    for step in range(EG_STEPS + 1):
        e0, e1, e2 = jnp.exp2(-g0), jnp.exp2(-g1), jnp.exp2(-g2)
        inverse = 1.0 / (e0 + e1 + e2)
        if step < EG_STEPS:
            g0 = g0 + (m00 * e0 + m01 * e1 + m02 * e2) * inverse
            g1 = g1 + (m01 * e0 + m11 * e1 + m12 * e2) * inverse
            g2 = g2 + (m02 * e0 + m12 * e1 + m22 * e2) * inverse
    return e0 * inverse, e1 * inverse, e2 * inverse


def write_shares(weights, main, rem, rows, out_ref):
    w0, w1, w2 = weights
    lane = lax.broadcasted_iota(jnp.int32, (8, 128), 1)
    rem_task, row_task = lane // 32, (lane % 24) // 8
    out_ref[0] = jnp.where(lane == 0, w0, jnp.where(lane == 1, w1, w2))
    rows = rows * jnp.where(row_task == 0, w0, jnp.where(row_task == 1, w1, w2))
    rows = rows + pltpu.roll(rows, 120, 1) + pltpu.roll(rows, 112, 1)
    out_ref[1] = rows
    out_ref[2] = w0 * main[0] + w1 * main[1] + w2 * main[2]
    rem = rem * jnp.where(rem_task == 0, w0, jnp.where(rem_task == 1, w1, w2))
    out_ref[3] = rem + pltpu.roll(rem, 96, 1) + pltpu.roll(rem, 64, 1)


def finish_kernel(tiles_ref, alpha_ref, ga_ref, gb_ref):
    alpha_ref[...] = tiles_ref[0, 0:1, 0:3]
    rows = tiles_ref[1].T
    ga_ref[...] = jnp.concatenate([rows[24 * k : 24 * k + 8, :] for k in range(5)], axis=1)
    gb_ref[:, 0:128] = tiles_ref[2]
    gb_ref[:, 128:160] = tiles_ref[3, :, 0:32]


def dot_t(lhs, rhs):
    return lax.dot_general(lhs, rhs, (((1,), (1,)), ((), ())), preferred_element_type=jnp.float32)


def dot_n(lhs, rhs):
    return jnp.dot(lhs, rhs, preferred_element_type=jnp.float32)


def gelu_and_slope(pre_act):
    square = pre_act * pre_act
    tanh = jnp.tanh(GELU_SCALE * pre_act * (1.0 + GELU_CUBE * square))
    cdf = 0.5 + 0.5 * tanh
    bell = (0.5 * GELU_SCALE) * (1.0 - tanh * tanh) * (1.0 + (3.0 * GELU_CUBE) * square)
    return pre_act * cdf, cdf + pre_act * bell


def logit_errors(logits, labels, num_classes):
    by_class = logits.T
    errors = []
    for t in range(NUM_TASKS):
        rows = by_class[16 * t : 16 * t + 16, :]
        cls = lax.broadcasted_iota(jnp.int32, rows.shape, 0)
        rows = jnp.where(cls < num_classes, rows, -jnp.inf)
        expo = jnp.exp(rows - jnp.max(rows, axis=0, keepdims=True))
        probs = expo / jnp.sum(expo, axis=0, keepdims=True)
        errors.append(probs - jnp.where(cls == labels[t : t + 1, :], 1.0, 0.0))
    errors.append(jnp.zeros((128 - 16 * NUM_TASKS, logits.shape[0]), jnp.float32))
    return jnp.concatenate(errors, axis=0).T


def pack_share_columns(main_cols, dest):
    first = 160 * dest // 128
    shift = 160 * dest - 128 * first
    main, rem = [], []
    for cols in main_cols:
        left = cols[:, 128 * first : 128 * first + 128]
        right = cols[:, 128 * first + 128 : 128 * first + 256]
        lane = lax.broadcasted_iota(jnp.int32, left.shape, 1)
        if shift == 0:
            main.append(left)
            rem.append(right)
        else:
            left, right = pltpu.roll(left, 128 - shift, 1), pltpu.roll(right, 128 - shift, 1)
            main.append(jnp.where(lane < 128 - shift, left, right))
            rem.append(right)
    lane = lax.broadcasted_iota(jnp.int32, (8, 128), 1)
    tail = jnp.where(lane < 32, rem[0], 0.0)
    tail = jnp.where(lane // 32 == 1, pltpu.roll(rem[1], 32, 1), tail)
    tail = jnp.where(lane // 32 == 2, pltpu.roll(rem[2], 64, 1), tail)
    return main, tail


def step_kernel(
    n, tok_total, num_classes,
    x_hbm, y_hbm, w1_hbm, w2_hbm, at_hbm, bm_hbm, ht_hbm,
    out_ref,
    x, y, w1, w2, at, bm, ht, slope, pre, z_acc, x_t, u_diag, bm_rep, hcat, err, dz, dp, du_acc,
    send_b, recv_b, sum_b, recv_z, send_a, recv_a, gram_send, gram_recv,
    in_sem, w1_sem, w2_sem, bsend_sem, brecv_sem, zsend_sem, zrecv_sem, asend_sem, arecv_sem, gsend_sem, grecv_sem,
):
    bf16, f32 = jnp.bfloat16, jnp.float32
    me = lax.axis_index("data")
    plane, spot = me // PLANE, me % PLANE
    planes = n // PLANE
    d_model, d_ff = w1_hbm.shape
    toks = x_hbm.shape[0]
    fwd_steps = d_ff // FWD_COLS

    small = [
        pltpu.make_async_copy(src, dst, in_sem.at[k])
        for k, (src, dst) in enumerate([(x_hbm, x), (at_hbm, at), (bm_hbm, bm), (ht_hbm, ht), (y_hbm, y)])
    ]
    def span(j):
        return pl.ds(pl.multiple_of(j * FWD_COLS, FWD_COLS), FWD_COLS)

    def w1_copy(j):
        return pltpu.make_async_copy(w1_hbm.at[:, span(j)], w1.at[:, span(j)], w1_sem.at[j])

    def w2_copy(j):
        return pltpu.make_async_copy(w2_hbm.at[span(j), :], w2.at[span(j), :], w2_sem.at[j])

    for copy in small:
        copy.start()
    w1_copy(0).start()

    def fetch(j, carry):
        w1_copy(j).start()
        w2_copy(j - 1).start()
        return carry

    lax.fori_loop(1, fwd_steps, fetch, 0)
    w2_copy(fwd_steps - 1).start()

    barrier = pltpu.get_barrier_semaphore()

    def greet(k, carry):
        pl.semaphore_signal(barrier, inc=1, device_id=(lax.rem(me + k, n),), device_id_type=MESH)
        return carry

    lax.fori_loop(1, n, greet, 0)

    for copy in small:
        copy.wait()
    low_rank = dot_t(x[...], at[...]).astype(bf16)

    def up_project(j):
        return dot_n(x[...], w1[:, span(j)]) + dot_n(low_rank, bm[:, span(j)])

    def activate(j):
        act, slope_tile = gelu_and_slope(pre[...])
        slope[:, span(j)] = slope_tile
        return act.astype(bf16)

    u_t = dot_t(at[...], x[...])
    blank = jnp.zeros_like(u_t)
    u_diag[...] = jnp.concatenate(
        [jnp.concatenate([u_t if s == t else blank for s in range(NUM_TASKS)], axis=1) for t in range(NUM_TASKS)], axis=0
    ).astype(bf16)
    bm_rep[...] = jnp.concatenate([bm[...].astype(f32)] * 16, axis=0).astype(bf16)
    gap = jnp.zeros((16 - num_classes, d_model), f32)
    heads = [part for t in range(NUM_TASKS) for part in (ht[t].astype(f32), gap)]
    hcat[...] = jnp.concatenate(heads + [jnp.zeros((128 - 16 * NUM_TASKS, d_model), f32)], axis=0).astype(bf16)
    x_t[...] = x[...].astype(f32).T.astype(bf16)

    z_acc[...] = jnp.zeros_like(z_acc)
    w1_copy(0).wait()
    pre[...] = up_project(0)

    def forward(j, carry):
        w1_copy(j + 1).wait()
        w2_copy(j).wait()
        act = activate(j)
        pre[...] = up_project(j + 1)
        z_acc[...] += dot_n(act, w2[span(j), :])
        return carry

    lax.fori_loop(0, fwd_steps - 1, forward, 0)
    w2_copy(fwd_steps - 1).wait()
    z_acc[...] += dot_n(activate(fwd_steps - 1), w2[span(fwd_steps - 1), :])

    trunk = (x[...].astype(f32) + z_acc[...]).astype(bf16)
    errors = logit_errors(dot_t(trunk, hcat[...]), y[...], num_classes)
    lane = lax.broadcasted_iota(jnp.int32, (toks, 128), 1)
    for t in range(NUM_TASKS):
        err[pl.ds(t * toks, toks), :] = jnp.where(lane // 16 == t, errors, 0.0).astype(bf16)
    dz[...] = dot_n(err[...], hcat[...]).astype(bf16)
    pl.semaphore_wait(barrier, n - 1)
    SEND_ON = True

    def plane_send(i):
        if not SEND_ON:
            return

        def send(k):
            to = lax.rem(spot + k, PLANE)
            pltpu.make_async_remote_copy(
                src_ref=send_b.at[i, to], dst_ref=recv_b.at[i, spot], send_sem=bsend_sem, recv_sem=brecv_sem.at[i],
                device_id=(plane * PLANE + to,), device_id_type=MESH,
            ).start()

        for k in range(1, PLANE):
            send(k)
        recv_b[i, spot] = send_b[i, spot]

    def plane_wait(i):
        pltpu.make_async_remote_copy(
            src_ref=send_b.at[i, pl.ds(0, PLANE - 1)], dst_ref=recv_b.at[i, pl.ds(0, PLANE - 1)], send_sem=bsend_sem, recv_sem=brecv_sem.at[i],
            device_id=(lax.rem(me + 1, n),), device_id_type=MESH,
        ).wait_recv()

    def across_send(i):
        if not SEND_ON:
            return
        plane_wait(i)
        sum_b[i] = jnp.sum(recv_b[i], axis=0)
        pltpu.make_async_remote_copy(
            src_ref=sum_b.at[i], dst_ref=recv_z.at[i], send_sem=zsend_sem, recv_sem=zrecv_sem,
            device_id=(lax.rem(plane + 1 + i, planes) * PLANE + spot,), device_id_type=MESH,
        ).start()

    def chunk_cols(i):
        chunk = lax.rem(plane + 1 + i, planes)
        return pl.ds(pl.multiple_of(chunk * BWD_COLS, BWD_COLS), BWD_COLS)

    def back_project(i):
        cols = chunk_cols(i)
        d_hidden = dot_t(dz[...], w2[cols, :])
        slope_tile = slope[:, cols]
        for t in range(NUM_TASKS):
            dp[pl.ds(t * toks, toks), :] = (d_hidden[t * toks : (t + 1) * toks, :] * slope_tile).astype(bf16)

    def low_rank_grad(i):
        du_acc[...] += dot_t(dp[...], bm_rep[:, chunk_cols(i)])

    def adapter_grad(i):
        grads = dot_n(u_diag[...], dp[...])
        for to in range(PLANE):
            main, tail = pack_share_columns([grads[8 * t : 8 * t + 8, :] for t in range(NUM_TASKS)], to)
            for t in range(NUM_TASKS):
                send_b[i, to, t] = main[t]
            send_b[i, to, NUM_TASKS] = tail

    du_acc[...] = jnp.zeros_like(du_acc)

    def backward(i, carry):
        back_project(i)
        low_rank_grad(i)
        adapter_grad(i)
        plane_send(i)

        @pl.when(i >= 1)
        def _():
            across_send(i - 1)

        return carry

    lax.fori_loop(0, planes, backward, 0)

    lane = lax.broadcasted_iota(jnp.int32, (toks, 128), 1)
    du = du_acc[2 * toks :, :]
    for t in range(NUM_TASKS - 1):
        du = jnp.where((lane // 8) % NUM_TASKS == t, du_acc[t * toks : (t + 1) * toks, :], du)
    rows_a = dot_n(x_t[...], du.astype(bf16)).reshape(n, 5, 8, 128)
    lane = lax.broadcasted_iota(jnp.int32, (n, 8, 128), 2)
    packed = jnp.where(lane < 120, rows_a[:, 4], 0.0)
    for k in range(4):
        packed = jnp.where(lane // 24 == k, rows_a[:, k], packed)
    send_a[...] = packed

    def send_rows(k, carry):
        to = lax.rem(me + k, n)
        pltpu.make_async_remote_copy(
            src_ref=send_a.at[to], dst_ref=recv_a.at[me], send_sem=asend_sem, recv_sem=arecv_sem,
            device_id=(to,), device_id_type=MESH,
        ).start()
        return carry

    lax.fori_loop(PLANE, n, send_rows, 0)
    lax.fori_loop(1, PLANE, send_rows, 0)
    recv_a[me] = send_a[me]

    plane_wait(planes - 1)
    every_z = pltpu.make_async_remote_copy(
        src_ref=sum_b, dst_ref=recv_z, send_sem=zsend_sem, recv_sem=zrecv_sem, device_id=(lax.rem(me + 1, n),), device_id_type=MESH
    )
    every_z.wait_recv()
    share_b = (jnp.sum(recv_b[planes - 1], axis=0) + jnp.sum(recv_z[...], axis=0)) / tok_total
    main, rem = (share_b[0], share_b[1], share_b[2]), share_b[3]
    every_a = pltpu.make_async_remote_copy(
        src_ref=send_a.at[pl.ds(0, n - 1)], dst_ref=recv_a.at[pl.ds(0, n - 1)], send_sem=asend_sem, recv_sem=arecv_sem,
        device_id=(lax.rem(me + 1, n),), device_id_type=MESH,
    )
    every_a.wait_recv()
    rows = jnp.sum(recv_a[...], axis=0) / tok_total
    gram_row = local_gram(main, rem, rows)
    gram_send[...] = gram_row
    gram_recv[me] = gram_row

    def send_gram(k, carry):
        pltpu.make_async_remote_copy(
            src_ref=gram_send, dst_ref=gram_recv.at[me], send_sem=gsend_sem, recv_sem=grecv_sem,
            device_id=(lax.rem(me + k, n),), device_id_type=MESH,
        ).start()
        return carry

    lax.fori_loop(PLANE, n, send_gram, 0)
    lax.fori_loop(1, PLANE, send_gram, 0)
    every_gram = pltpu.make_async_remote_copy(
        src_ref=gram_recv.at[pl.ds(0, n - 1)], dst_ref=gram_recv.at[pl.ds(0, n - 1)], send_sem=gsend_sem, recv_sem=grecv_sem,
        device_id=(lax.rem(me + 1, n),), device_id_type=MESH,
    )
    pltpu.make_async_remote_copy(
        src_ref=send_b.at[:, pl.ds(0, PLANE - 1)], dst_ref=recv_b.at[:, pl.ds(0, PLANE - 1)], send_sem=bsend_sem, recv_sem=brecv_sem.at[0],
        device_id=(lax.rem(me + 1, n),), device_id_type=MESH,
    ).wait_send()
    every_z.wait_send()
    every_a.wait_send()
    every_gram.wait_recv()
    weights = solve_weights(jnp.sum(gram_recv[...], axis=0))
    write_shares(weights, main, rem, rows, out_ref)
    every_gram.wait_send()


def solution(mesh):
    num_dev = mesh.shape["data"]

    def device_step(tokens, labels, w_one, w_two, adapter_a, adapter_b, task_heads):
        toks, d_model = tokens.shape
        d_ff = w_one.shape[1]
        planes = num_dev // PLANE
        fwd_steps = d_ff // FWD_COLS
        bf16, f32 = jnp.bfloat16, jnp.float32
        dma = pltpu.SemaphoreType.DMA
        vmem = pl.BlockSpec(memory_space=pltpu.VMEM)
        hbm = pl.BlockSpec(memory_space=pltpu.HBM)
        adapter_t = adapter_a.T
        heads_t = task_heads.transpose(0, 2, 1)
        tiles = pl.pallas_call(
            functools.partial(step_kernel, num_dev, float(toks * num_dev), task_heads.shape[2]),
            out_shape=jax.ShapeDtypeStruct((4, 8, 128), f32),
            in_specs=[hbm] * 7,
            out_specs=vmem,
            scratch_shapes=[
                pltpu.VMEM(tokens.shape, bf16),
                pltpu.VMEM(labels.shape, jnp.int32),
                pltpu.VMEM(w_one.shape, bf16),
                pltpu.VMEM(w_two.shape, bf16),
                pltpu.VMEM(adapter_t.shape, bf16),
                pltpu.VMEM(adapter_b.shape, bf16),
                pltpu.VMEM(heads_t.shape, bf16),
                pltpu.VMEM((toks, d_ff), f32),
                pltpu.VMEM((toks, FWD_COLS), f32),
                pltpu.VMEM((toks, d_model), f32),
                pltpu.VMEM((d_model, toks), bf16),
                pltpu.VMEM((8 * NUM_TASKS, NUM_TASKS * toks), bf16),
                pltpu.VMEM((128, d_ff), bf16),
                pltpu.VMEM((128, d_model), bf16),
                pltpu.VMEM((NUM_TASKS * toks, 128), bf16),
                pltpu.VMEM((NUM_TASKS * toks, d_model), bf16),
                pltpu.VMEM((NUM_TASKS * toks, BWD_COLS), bf16),
                pltpu.VMEM((NUM_TASKS * toks, 128), f32),
                pltpu.VMEM((planes, PLANE, 4, 8, 128), f32),
                pltpu.VMEM((planes, PLANE, 4, 8, 128), f32),
                pltpu.VMEM((planes - 1, 4, 8, 128), f32),
                pltpu.VMEM((planes - 1, 4, 8, 128), f32),
                pltpu.VMEM((num_dev, 8, 128), f32),
                pltpu.VMEM((num_dev, 8, 128), f32),
                pltpu.VMEM((1, 128), f32),
                pltpu.VMEM((num_dev, 1, 128), f32),
                dma((5,)),
                dma((fwd_steps,)),
                dma((fwd_steps,)),
                dma,
                dma((planes,)),
                dma,
                dma,
                dma,
                dma,
                dma,
                dma,
            ],
            compiler_params=pltpu.CompilerParams(collective_id=0, has_side_effects=True, vmem_limit_bytes=52 * 1024 * 1024),
            name="grad_step",
        )(*[pltpu.with_memory_space_constraint(arg, pltpu.HBM) for arg in (tokens, labels, w_one, w_two, adapter_t, adapter_b, heads_t)])
        alpha, comb_at, comb_b = pl.pallas_call(
            finish_kernel,
            out_shape=(
                jax.ShapeDtypeStruct((1, NUM_TASKS), f32),
                jax.ShapeDtypeStruct((8, d_model // num_dev), f32),
                jax.ShapeDtypeStruct((8, d_ff // num_dev), f32),
            ),
            in_specs=[vmem],
            out_specs=(vmem, vmem, vmem),
            compiler_params=pltpu.CompilerParams(vmem_limit_bytes=1024 * 1024),
            name="write_out",
        )(tiles)
        return alpha[0], comb_at.T, comb_b

    return jax.shard_map(device_step, mesh=mesh, in_specs=(P("data", None), P(None, "data"), P(), P(), P(), P(), P()), out_specs=(P(), P("data", None), P(None, "data")), check_vma=False)
```

```python
import functools

import jax
import jax.numpy as jnp
from jax import lax
from jax.experimental import pallas as pl
from jax.experimental.pallas import tpu as pltpu
from jax.sharding import PartitionSpec as P

EG_STEPS = 20
FWD_COLS = 512
BWD_COLS = 1280
NUM_TASKS = 3
PLANE = 8
GELU_SCALE = 0.7978845608028654
GELU_CUBE = 0.044715
MESH = pl.DeviceIdType.MESH


def full_sum(tile):
    return jnp.sum(jnp.sum(tile, axis=0, keepdims=True), axis=1, keepdims=True)


def local_gram(main, rem, rows):
    lane = lax.broadcasted_iota(jnp.int32, (8, 128), 1)
    rem_task = lane // 32
    row_task = (lane % 24) // 8
    rem_1, rem_2 = pltpu.roll(rem, 96, 1), pltpu.roll(rem, 64, 1)
    row_1, row_2 = pltpu.roll(rows, 120, 1), pltpu.roll(rows, 112, 1)

    def entry(t, s, rem_other, row_other):
        tile = main[t] * main[s]
        tile = tile + jnp.where(rem_task == t, rem * rem_other, 0.0)
        return full_sum(tile + jnp.where(row_task == t, rows * row_other, 0.0))

    entries = [entry(0, 0, rem, rows), entry(1, 1, rem, rows), entry(2, 2, rem, rows)]
    entries += [entry(0, 1, rem_1, row_1), entry(1, 2, rem_1, row_1), entry(0, 2, rem_2, row_2)]
    lane_row = lax.broadcasted_iota(jnp.int32, (1, 128), 1)
    gram_row = jnp.zeros((1, 128), jnp.float32)
    for k, value in enumerate(entries):
        gram_row = jnp.where(lane_row == k, value, gram_row)
    return gram_row


def solve_weights(gram_row):
    lane_row = lax.broadcasted_iota(jnp.int32, (1, 128), 1)
    m00, m11, m22, m01, m12, m02 = [jnp.sum(jnp.where(lane_row == k, gram_row, 0.0), axis=1, keepdims=True) for k in range(6)]
    to_exponent = 1.4426950408889634 / ((m00 + m11 + m22) / 3.0)
    m00, m11, m22, m01, m12, m02 = [m * to_exponent for m in (m00, m11, m22, m01, m12, m02)]

    g0 = g1 = g2 = jnp.zeros((1, 1), jnp.float32)
    for step in range(EG_STEPS + 1):
        e0, e1, e2 = jnp.exp2(-g0), jnp.exp2(-g1), jnp.exp2(-g2)
        inverse = 1.0 / (e0 + e1 + e2)
        if step < EG_STEPS:
            g0 = g0 + (m00 * e0 + m01 * e1 + m02 * e2) * inverse
            g1 = g1 + (m01 * e0 + m11 * e1 + m12 * e2) * inverse
            g2 = g2 + (m02 * e0 + m12 * e1 + m22 * e2) * inverse
    return e0 * inverse, e1 * inverse, e2 * inverse


def write_shares(weights, main, rem, rows, out_ref):
    w0, w1, w2 = weights
    lane = lax.broadcasted_iota(jnp.int32, (8, 128), 1)
    rem_task, row_task = lane // 32, (lane % 24) // 8
    out_ref[0] = jnp.where(lane == 0, w0, jnp.where(lane == 1, w1, w2))
    rows = rows * jnp.where(row_task == 0, w0, jnp.where(row_task == 1, w1, w2))
    rows = rows + pltpu.roll(rows, 120, 1) + pltpu.roll(rows, 112, 1)
    out_ref[1] = rows
    out_ref[2] = w0 * main[0] + w1 * main[1] + w2 * main[2]
    rem = rem * jnp.where(rem_task == 0, w0, jnp.where(rem_task == 1, w1, w2))
    out_ref[3] = rem + pltpu.roll(rem, 96, 1) + pltpu.roll(rem, 64, 1)


def finish_kernel(tiles_ref, alpha_ref, ga_ref, gb_ref):
    alpha_ref[...] = tiles_ref[0, 0:1, 0:3]
    rows = tiles_ref[1].T
    ga_ref[...] = jnp.concatenate([rows[24 * k : 24 * k + 8, :] for k in range(5)], axis=1)
    gb_ref[:, 0:128] = tiles_ref[2]
    gb_ref[:, 128:160] = tiles_ref[3, :, 0:32]


def dot_t(lhs, rhs):
    return lax.dot_general(lhs, rhs, (((1,), (1,)), ((), ())), preferred_element_type=jnp.float32)


def dot_n(lhs, rhs):
    return jnp.dot(lhs, rhs, preferred_element_type=jnp.float32)


def gelu_and_slope(pre_act):
    square = pre_act * pre_act
    tanh = jnp.tanh(GELU_SCALE * pre_act * (1.0 + GELU_CUBE * square))
    cdf = 0.5 + 0.5 * tanh
    bell = (0.5 * GELU_SCALE) * (1.0 - tanh * tanh) * (1.0 + (3.0 * GELU_CUBE) * square)
    return pre_act * cdf, cdf + pre_act * bell


def logit_errors(logits, labels, num_classes):
    by_class = logits.T
    errors = []
    for t in range(NUM_TASKS):
        rows = by_class[16 * t : 16 * t + 16, :]
        cls = lax.broadcasted_iota(jnp.int32, rows.shape, 0)
        rows = jnp.where(cls < num_classes, rows, -jnp.inf)
        expo = jnp.exp(rows - jnp.max(rows, axis=0, keepdims=True))
        probs = expo / jnp.sum(expo, axis=0, keepdims=True)
        errors.append(probs - jnp.where(cls == labels[t : t + 1, :], 1.0, 0.0))
    errors.append(jnp.zeros((128 - 16 * NUM_TASKS, logits.shape[0]), jnp.float32))
    return jnp.concatenate(errors, axis=0).T


def pack_share_columns(main_cols, dest):
    first = 160 * dest // 128
    shift = 160 * dest - 128 * first
    main, rem = [], []
    for cols in main_cols:
        left = cols[:, 128 * first : 128 * first + 128]
        right = cols[:, 128 * first + 128 : 128 * first + 256]
        lane = lax.broadcasted_iota(jnp.int32, left.shape, 1)
        if shift == 0:
            main.append(left)
            rem.append(right)
        else:
            left, right = pltpu.roll(left, 128 - shift, 1), pltpu.roll(right, 128 - shift, 1)
            main.append(jnp.where(lane < 128 - shift, left, right))
            rem.append(right)
    lane = lax.broadcasted_iota(jnp.int32, (8, 128), 1)
    tail = jnp.where(lane < 32, rem[0], 0.0)
    tail = jnp.where(lane // 32 == 1, pltpu.roll(rem[1], 32, 1), tail)
    tail = jnp.where(lane // 32 == 2, pltpu.roll(rem[2], 64, 1), tail)
    return main, tail


def step_kernel(
    n, tok_total, num_classes,
    x_hbm, y_hbm, w1_hbm, w2_hbm, at_hbm, bm_hbm, ht_hbm,
    out_ref,
    x, y, w1, w2, at, bm, ht, slope, pre, held, z_acc, x_t, u_diag, bm_rep, hcat, err, dz, dp, du_acc,
    send_b, recv_b, sum_b, recv_z, send_a, recv_a, gram_send, gram_recv,
    in_sem, w1_sem, w2_sem, bsend_sem, brecv_sem, zsend_sem, zrecv_sem, asend_sem, arecv_sem, gsend_sem, grecv_sem,
):
    bf16, f32 = jnp.bfloat16, jnp.float32
    me = lax.axis_index("data")
    plane, spot = me // PLANE, me % PLANE
    planes = n // PLANE
    d_model, d_ff = w1_hbm.shape
    toks = x_hbm.shape[0]
    fwd_steps = d_ff // FWD_COLS

    small = [
        pltpu.make_async_copy(src, dst, in_sem.at[k])
        for k, (src, dst) in enumerate([(x_hbm, x), (at_hbm, at), (bm_hbm, bm), (ht_hbm, ht), (y_hbm, y)])
    ]
    def span(j):
        return pl.ds(pl.multiple_of(j * FWD_COLS, FWD_COLS), FWD_COLS)

    def w1_copy(j):
        return pltpu.make_async_copy(w1_hbm.at[:, span(j)], w1.at[:, span(j)], w1_sem.at[j])

    def w2_copy(j):
        return pltpu.make_async_copy(w2_hbm.at[span(j), :], w2.at[span(j), :], w2_sem.at[j])

    for copy in small:
        copy.start()
    w1_copy(0).start()

    def fetch(j, carry):
        w1_copy(j).start()
        w2_copy(j - 1).start()
        return carry

    lax.fori_loop(1, fwd_steps, fetch, 0)
    w2_copy(fwd_steps - 1).start()

    barrier = pltpu.get_barrier_semaphore()

    def greet(k, carry):
        pl.semaphore_signal(barrier, inc=1, device_id=(lax.rem(me + k, n),), device_id_type=MESH)
        return carry

    lax.fori_loop(1, n, greet, 0)

    for copy in small:
        copy.wait()
    low_rank = dot_t(x[...], at[...]).astype(bf16)

    def up_project(j):
        return dot_n(x[...], w1[:, span(j)]) + dot_n(low_rank, bm[:, span(j)])

    def activate(j):
        act, slope_tile = gelu_and_slope(pre[...])
        slope[:, span(j)] = slope_tile
        return act.astype(bf16)

    u_t = dot_t(at[...], x[...])
    blank = jnp.zeros_like(u_t)
    u_diag[...] = jnp.concatenate(
        [jnp.concatenate([u_t if s == t else blank for s in range(NUM_TASKS)], axis=1) for t in range(NUM_TASKS)], axis=0
    ).astype(bf16)
    bm_rep[...] = jnp.concatenate([bm[...].astype(f32)] * 16, axis=0).astype(bf16)
    gap = jnp.zeros((16 - num_classes, d_model), f32)
    heads = [part for t in range(NUM_TASKS) for part in (ht[t].astype(f32), gap)]
    hcat[...] = jnp.concatenate(heads + [jnp.zeros((128 - 16 * NUM_TASKS, d_model), f32)], axis=0).astype(bf16)
    x_t[...] = x[...].astype(f32).T.astype(bf16)

    z_acc[...] = jnp.zeros_like(z_acc)
    w1_copy(0).wait()
    pre[...] = up_project(0)
    held[...] = activate(0)
    w1_copy(1).wait()
    pre[...] = up_project(1)

    def forward(j, carry):
        w1_copy(j + 1).wait()
        w2_copy(j - 1).wait()
        z_acc[...] += dot_n(held[...], w2[span(j - 1), :])
        act = activate(j)
        pre[...] = up_project(j + 1)
        held[...] = act
        return carry

    lax.fori_loop(1, fwd_steps - 1, forward, 0)
    w2_copy(fwd_steps - 2).wait()
    w2_copy(fwd_steps - 1).wait()
    z_acc[...] += dot_n(held[...], w2[span(fwd_steps - 2), :])
    z_acc[...] += dot_n(activate(fwd_steps - 1), w2[span(fwd_steps - 1), :])

    trunk = (x[...].astype(f32) + z_acc[...]).astype(bf16)
    errors = logit_errors(dot_t(trunk, hcat[...]), y[...], num_classes)
    lane = lax.broadcasted_iota(jnp.int32, (toks, 128), 1)
    for t in range(NUM_TASKS):
        err[pl.ds(t * toks, toks), :] = jnp.where(lane // 16 == t, errors, 0.0).astype(bf16)
    dz[...] = dot_n(err[...], hcat[...]).astype(bf16)
    pl.semaphore_wait(barrier, n - 1)
    SEND_ON = True

    def plane_send(i):
        if not SEND_ON:
            return

        def send(k):
            to = lax.rem(spot + k, PLANE)
            pltpu.make_async_remote_copy(
                src_ref=send_b.at[i, to], dst_ref=recv_b.at[i, spot], send_sem=bsend_sem, recv_sem=brecv_sem.at[i],
                device_id=(plane * PLANE + to,), device_id_type=MESH,
            ).start()

        for k in range(1, PLANE):
            send(k)
        recv_b[i, spot] = send_b[i, spot]

    def plane_wait(i):
        pltpu.make_async_remote_copy(
            src_ref=send_b.at[i, pl.ds(0, PLANE - 1)], dst_ref=recv_b.at[i, pl.ds(0, PLANE - 1)], send_sem=bsend_sem, recv_sem=brecv_sem.at[i],
            device_id=(lax.rem(me + 1, n),), device_id_type=MESH,
        ).wait_recv()

    def across_send(i):
        if not SEND_ON:
            return
        plane_wait(i)
        sum_b[i] = jnp.sum(recv_b[i], axis=0)
        pltpu.make_async_remote_copy(
            src_ref=sum_b.at[i], dst_ref=recv_z.at[i], send_sem=zsend_sem, recv_sem=zrecv_sem,
            device_id=(lax.rem(plane + 1 + i, planes) * PLANE + spot,), device_id_type=MESH,
        ).start()

    def chunk_cols(i):
        chunk = lax.rem(plane + 1 + i, planes)
        return pl.ds(pl.multiple_of(chunk * BWD_COLS, BWD_COLS), BWD_COLS)

    def back_project(i):
        cols = chunk_cols(i)
        d_hidden = dot_t(dz[...], w2[cols, :])
        slope_tile = slope[:, cols]
        for t in range(NUM_TASKS):
            dp[pl.ds(t * toks, toks), :] = (d_hidden[t * toks : (t + 1) * toks, :] * slope_tile).astype(bf16)

    def low_rank_grad(i):
        du_acc[...] += dot_t(dp[...], bm_rep[:, chunk_cols(i)])

    def adapter_grad(i):
        grads = dot_n(u_diag[...], dp[...])
        for to in range(PLANE):
            main, tail = pack_share_columns([grads[8 * t : 8 * t + 8, :] for t in range(NUM_TASKS)], to)
            for t in range(NUM_TASKS):
                send_b[i, to, t] = main[t]
            send_b[i, to, NUM_TASKS] = tail

    du_acc[...] = jnp.zeros_like(du_acc)

    def backward(i, carry):
        back_project(i)
        low_rank_grad(i)
        adapter_grad(i)
        plane_send(i)

        @pl.when(i >= 1)
        def _():
            across_send(i - 1)

        return carry

    lax.fori_loop(0, planes, backward, 0)

    lane = lax.broadcasted_iota(jnp.int32, (toks, 128), 1)
    du = du_acc[2 * toks :, :]
    for t in range(NUM_TASKS - 1):
        du = jnp.where((lane // 8) % NUM_TASKS == t, du_acc[t * toks : (t + 1) * toks, :], du)
    rows_a = dot_n(x_t[...], du.astype(bf16)).reshape(n, 5, 8, 128)
    lane = lax.broadcasted_iota(jnp.int32, (n, 8, 128), 2)
    packed = jnp.where(lane < 120, rows_a[:, 4], 0.0)
    for k in range(4):
        packed = jnp.where(lane // 24 == k, rows_a[:, k], packed)
    send_a[...] = packed

    def send_rows(k, carry):
        to = lax.rem(me + k, n)
        pltpu.make_async_remote_copy(
            src_ref=send_a.at[to], dst_ref=recv_a.at[me], send_sem=asend_sem, recv_sem=arecv_sem,
            device_id=(to,), device_id_type=MESH,
        ).start()
        return carry

    lax.fori_loop(PLANE, n, send_rows, 0)
    lax.fori_loop(1, PLANE, send_rows, 0)
    recv_a[me] = send_a[me]

    plane_wait(planes - 1)
    every_z = pltpu.make_async_remote_copy(
        src_ref=sum_b, dst_ref=recv_z, send_sem=zsend_sem, recv_sem=zrecv_sem, device_id=(lax.rem(me + 1, n),), device_id_type=MESH
    )
    every_z.wait_recv()
    share_b = (jnp.sum(recv_b[planes - 1], axis=0) + jnp.sum(recv_z[...], axis=0)) / tok_total
    main, rem = (share_b[0], share_b[1], share_b[2]), share_b[3]
    every_a = pltpu.make_async_remote_copy(
        src_ref=send_a.at[pl.ds(0, n - 1)], dst_ref=recv_a.at[pl.ds(0, n - 1)], send_sem=asend_sem, recv_sem=arecv_sem,
        device_id=(lax.rem(me + 1, n),), device_id_type=MESH,
    )
    every_a.wait_recv()
    rows = jnp.sum(recv_a[...], axis=0) / tok_total
    gram_row = local_gram(main, rem, rows)
    gram_send[...] = gram_row
    gram_recv[me] = gram_row

    def send_gram(k, carry):
        pltpu.make_async_remote_copy(
            src_ref=gram_send, dst_ref=gram_recv.at[me], send_sem=gsend_sem, recv_sem=grecv_sem,
            device_id=(lax.rem(me + k, n),), device_id_type=MESH,
        ).start()
        return carry

    lax.fori_loop(PLANE, n, send_gram, 0)
    lax.fori_loop(1, PLANE, send_gram, 0)
    every_gram = pltpu.make_async_remote_copy(
        src_ref=gram_recv.at[pl.ds(0, n - 1)], dst_ref=gram_recv.at[pl.ds(0, n - 1)], send_sem=gsend_sem, recv_sem=grecv_sem,
        device_id=(lax.rem(me + 1, n),), device_id_type=MESH,
    )
    pltpu.make_async_remote_copy(
        src_ref=send_b.at[:, pl.ds(0, PLANE - 1)], dst_ref=recv_b.at[:, pl.ds(0, PLANE - 1)], send_sem=bsend_sem, recv_sem=brecv_sem.at[0],
        device_id=(lax.rem(me + 1, n),), device_id_type=MESH,
    ).wait_send()
    every_z.wait_send()
    every_a.wait_send()
    every_gram.wait_recv()
    weights = solve_weights(jnp.sum(gram_recv[...], axis=0))
    write_shares(weights, main, rem, rows, out_ref)
    every_gram.wait_send()


def solution(mesh):
    num_dev = mesh.shape["data"]

    def device_step(tokens, labels, w_one, w_two, adapter_a, adapter_b, task_heads):
        toks, d_model = tokens.shape
        d_ff = w_one.shape[1]
        planes = num_dev // PLANE
        fwd_steps = d_ff // FWD_COLS
        bf16, f32 = jnp.bfloat16, jnp.float32
        dma = pltpu.SemaphoreType.DMA
        vmem = pl.BlockSpec(memory_space=pltpu.VMEM)
        hbm = pl.BlockSpec(memory_space=pltpu.HBM)
        adapter_t = adapter_a.T
        heads_t = task_heads.transpose(0, 2, 1)
        tiles = pl.pallas_call(
            functools.partial(step_kernel, num_dev, float(toks * num_dev), task_heads.shape[2]),
            out_shape=jax.ShapeDtypeStruct((4, 8, 128), f32),
            in_specs=[hbm] * 7,
            out_specs=vmem,
            scratch_shapes=[
                pltpu.VMEM(tokens.shape, bf16),
                pltpu.VMEM(labels.shape, jnp.int32),
                pltpu.VMEM(w_one.shape, bf16),
                pltpu.VMEM(w_two.shape, bf16),
                pltpu.VMEM(adapter_t.shape, bf16),
                pltpu.VMEM(adapter_b.shape, bf16),
                pltpu.VMEM(heads_t.shape, bf16),
                pltpu.VMEM((toks, d_ff), f32),
                pltpu.VMEM((toks, FWD_COLS), f32),
                pltpu.VMEM((toks, FWD_COLS), bf16),
                pltpu.VMEM((toks, d_model), f32),
                pltpu.VMEM((d_model, toks), bf16),
                pltpu.VMEM((8 * NUM_TASKS, NUM_TASKS * toks), bf16),
                pltpu.VMEM((128, d_ff), bf16),
                pltpu.VMEM((128, d_model), bf16),
                pltpu.VMEM((NUM_TASKS * toks, 128), bf16),
                pltpu.VMEM((NUM_TASKS * toks, d_model), bf16),
                pltpu.VMEM((NUM_TASKS * toks, BWD_COLS), bf16),
                pltpu.VMEM((NUM_TASKS * toks, 128), f32),
                pltpu.VMEM((planes, PLANE, 4, 8, 128), f32),
                pltpu.VMEM((planes, PLANE, 4, 8, 128), f32),
                pltpu.VMEM((planes - 1, 4, 8, 128), f32),
                pltpu.VMEM((planes - 1, 4, 8, 128), f32),
                pltpu.VMEM((num_dev, 8, 128), f32),
                pltpu.VMEM((num_dev, 8, 128), f32),
                pltpu.VMEM((1, 128), f32),
                pltpu.VMEM((num_dev, 1, 128), f32),
                dma((5,)),
                dma((fwd_steps,)),
                dma((fwd_steps,)),
                dma,
                dma((planes,)),
                dma,
                dma,
                dma,
                dma,
                dma,
                dma,
            ],
            compiler_params=pltpu.CompilerParams(collective_id=0, has_side_effects=True, vmem_limit_bytes=52 * 1024 * 1024),
            name="grad_step",
        )(*[pltpu.with_memory_space_constraint(arg, pltpu.HBM) for arg in (tokens, labels, w_one, w_two, adapter_t, adapter_b, heads_t)])
        alpha, comb_at, comb_b = pl.pallas_call(
            finish_kernel,
            out_shape=(
                jax.ShapeDtypeStruct((1, NUM_TASKS), f32),
                jax.ShapeDtypeStruct((8, d_model // num_dev), f32),
                jax.ShapeDtypeStruct((8, d_ff // num_dev), f32),
            ),
            in_specs=[vmem],
            out_specs=(vmem, vmem, vmem),
            compiler_params=pltpu.CompilerParams(vmem_limit_bytes=1024 * 1024),
            name="write_out",
        )(tiles)
        return alpha[0], comb_at.T, comb_b

    return jax.shard_map(device_step, mesh=mesh, in_specs=(P("data", None), P(None, "data"), P(), P(), P(), P(), P()), out_specs=(P(), P("data", None), P(None, "data")), check_vma=False)
```
